128 devices in a mesh: pa: 128 (over z, y, x, core).
Axes of the slice: x: 4, y: 4, z: 4, core: 2. Of those that a mesh axis runs over, the one named last changes fastest.
Arguments:
- signal_real: float32 [67108864], P('pa'), may hold values from -6 to 6
- signal_imag: float32 [67108864], P('pa'), may hold values from -6 to 6
Outputs:
- spectrum_real: float32 [67108864], P('pa')
- spectrum_imag: float32 [67108864], P('pa')
The draws below stay inside these ranges and needn't reach their ends.
All inputs are finite; a program needn't handle non-finite values.
Results may differ from the reference program's by a relative error of at most 0.0003.
Values sent between devices are 32-bit elements.
A program may use at most 128 MiB of HBM per device.

```python
import jax
import jax.numpy as jnp

LENGTH = 67108864


def levels(own_key, extent, shards, low, largest):
    level, own = 1.0, jax.random.fold_in(own_key, 6)
    for dim, blocks in shards:
        draws = jnp.exp(jax.random.uniform(jax.random.fold_in(own, dim), (blocks,), jnp.float32, low / len(shards), largest / len(shards)))
        level = level * jnp.repeat(draws, extent[dim] // blocks).reshape([-1 if axis == dim else 1 for axis in range(len(extent))])
    return level


def noise(own_key, extent, width, most, cuts=(), kind=jnp.bfloat16):
    level = levels(own_key, extent, cuts, -0.22, 0.18) if cuts else 1.0
    drawn = jax.random.normal(own_key, extent, jnp.float32) * width * level
    return jnp.minimum(jnp.maximum(drawn, -most), most).astype(kind)


def setup_inputs(seed: int = 0) -> dict:
    splits = jax.random.split(jax.random.key(seed), 3)
    return {
        "signal_real": noise(splits[0], (LENGTH,), 1.0, 6.0, ((0, 128),), jnp.float32),
        "signal_imag": noise(splits[1], (LENGTH,), 1.0, 6.0, ((0, 128),), jnp.float32),
    }


def reference(signal_real, signal_imag):
    spectrum = jnp.fft.fft(signal_real + 1j * signal_imag, norm="ortho")
    return jnp.real(spectrum).astype(jnp.float32), jnp.imag(spectrum).astype(jnp.float32)
```

```python
import math

import jax
import jax.numpy as jnp
from jax import lax
from jax.experimental import pallas as pl
from jax.experimental.pallas import tpu as pltpu
from jax.sharding import PartitionSpec as P

MESH = pl.DeviceIdType.MESH
F32 = jnp.float32
BF16 = jnp.bfloat16
ROOT_HALF = math.sqrt(0.5)
ORDERS = ("zxy", "xyz", "yzx", "zxy", "xyz", "yzx", "zxy", "xyz")


def device(z, y, x, c):
    return ((z * 4 + y) * 4 + x) * 2 + c


def unit_root(phase, bits):
    phase = phase & ((1 << bits) - 1)
    quarter = (phase + (1 << (bits - 3))) >> (bits - 2)
    angle = (phase - (quarter << (bits - 2))).astype(F32) * (2.0 * math.pi / (1 << bits))
    square = angle * angle
    sine = angle * (1.0 + square * (-1 / 6 + square * (1 / 120 + square * (-1 / 5040 + square * (1 / 362880)))))
    cosine = 1.0 + square * (-1 / 2 + square * (1 / 24 + square * (-1 / 720 + square * (1 / 40320))))
    odd = (quarter & 1) == 1
    real = jnp.where(odd, sine, cosine)
    imag = jnp.where(odd, cosine, sine)
    real = jnp.where(((quarter + 1) & 2) == 2, -real, real)
    imag = jnp.where((quarter & 2) == 2, imag, -imag)
    return real, imag


def times(value, factor):
    (a, b), (c, d) = value, factor
    return a * c - b * d, a * d + b * c


def plus(a, b):
    return a[0] + b[0], a[1] + b[1]


def minus(a, b):
    return a[0] - b[0], a[1] - b[1]


def dft4(v):
    s, d = plus(v[0], v[2]), minus(v[0], v[2])
    t, u = plus(v[1], v[3]), minus(v[1], v[3])
    return [plus(s, t), (d[0] + u[1], d[1] - u[0]), minus(s, t), (d[0] - u[1], d[1] + u[0])]


def dft8(v):
    even, odd = dft4(v[0::2]), dft4(v[1::2])
    turned = [
        odd[0],
        ((odd[1][0] + odd[1][1]) * ROOT_HALF, (odd[1][1] - odd[1][0]) * ROOT_HALF),
        (odd[2][1], -odd[2][0]),
        ((odd[3][1] - odd[3][0]) * ROOT_HALF, (odd[3][0] + odd[3][1]) * -ROOT_HALF),
    ]
    return [plus(e, t) for e, t in zip(even, turned)] + [minus(e, t) for e, t in zip(even, turned)]


def split(value):
    high = value.astype(BF16)
    return high, (value - high.astype(F32)).astype(BF16)


def kernel(
    re_hbm, im_hbm, out_re, out_im,
    b1, b2, b3, b4, p0, p1, p2, p3, turn, out, z_hi, z_lo, g_hi, g_lo, h_hi, h_lo, lanes,
    own_sem, send_sem, recv_sem, last_sem, out_sem,
):
    me = lax.axis_index("pa")
    z, y, x, c = me // 32, (me // 8) % 4, (me // 2) % 4, me % 2
    inputs, outputs = (re_hbm, im_hbm), (out_re, out_im)

    barrier = pltpu.get_barrier_semaphore()
    peers = [device(z, (y + d) % 4, x, c) for d in (1, 2, 3)]
    peers += [device(z, y, (x + d) % 4, (c + t) % 2) for d in range(4) for t in range(2) if d + t]
    peers += [device((z + d) % 4, y, x, (c + t) % 2) for d in (1, 2, 3) for t in range(2)]
    for peer in peers:
        pl.semaphore_signal(barrier, inc=1, device_id=(peer,), device_id_type=MESH)
    pl.semaphore_wait(barrier, len(peers))

    def send(src, dst, stage, sem, peer):
        pltpu.make_async_remote_copy(
            src_ref=src, dst_ref=dst, send_sem=send_sem.at[stage], recv_sem=sem, device_id=(peer,), device_id_type=MESH
        ).start()

    def landed(ref, sem):
        pltpu.make_async_remote_copy(
            src_ref=ref, dst_ref=ref, send_sem=sem, recv_sem=sem, device_id=(me,), device_id_type=MESH
        ).wait_recv()

    for q in range(4):
        for part in range(2):

            @pl.loop(0, 8)
            def _(i):
                for d in (1, 3, 2):
                    to = (z + d) % 4
                    send(
                        inputs[part].at[to, :, i * 4 + q, 0],
                        b1.at[q, part, z, i],
                        0, recv_sem.at[0, q], device(to, y, x, c),
                    )
                pltpu.make_async_copy(
                    inputs[part].at[z, :, i * 4 + q, 0], b1.at[q, part, z, i], own_sem.at[q]
                ).start()

    s = z * 32 + c * 16 + x * 4 + y
    rows = lax.broadcasted_iota(jnp.int32, (128, 128), 0)
    cols = lax.broadcasted_iota(jnp.int32, (128, 128), 1)

    def matrix(phase, bits, scale, high, low):
        real, imag = unit_root(phase, bits)
        real, imag = real * scale, imag * scale
        for r, k, block in ((0, 0, real), (0, 1, -imag), (1, 0, imag), (1, 1, real)):
            hi, lo = split(block)
            high[r * 128 : (r + 1) * 128, k * 128 : (k + 1) * 128] = hi
            low[r * 128 : (r + 1) * 128, k * 128 : (k + 1) * 128] = lo

    matrix((rows * 128 + s) * cols, 14, 1.0, g_hi, g_lo)
    target = (rows & 96) + (rows & 3) * 8 + ((rows >> 2) & 3) * 2 + ((rows >> 4) & 1)
    matrix(target * cols, 7, 1.0 / 8192.0, h_hi, h_lo)
    lane_rows = lax.broadcasted_iota(jnp.int32, (32, 128), 0)
    lane_cols = lax.broadcasted_iota(jnp.int32, (32, 128), 1)
    lanes[0], lanes[1] = unit_root(lane_rows * lane_cols, 12)

    @pl.loop(0, 32)
    def _(f):
        real, imag = unit_root((rows * 128 + s) * (cols + f * 128), 26)
        turn[0, f] = real
        turn[1, f] = imag

    def scalar_root(phase, bits):
        return unit_root(jnp.full((8, 128), 1, jnp.int32) * phase, bits)

    turn_y = [scalar_root(k * y, 4) for k in range(4)]
    turn_x = [scalar_root((4 * k + y) * (2 * x + c), 7) for k in range(4)]

    def four(buf, q, factors):
        @pl.loop(0, 8)
        def _(i):
            v = [tuple(buf[q, p, k, i].reshape(4, 8, 128) for p in range(2)) for k in range(4)]
            v = [times(o, (w[0][None], w[1][None])) for o, w in zip(dft4(v), factors)]
            for k in range(4):
                for p in range(2):
                    buf[q, p, k, i] = v[k][p].reshape(32, 128)

    def step_z(q):
        landed(b1.at[q, :, pl.ds(0, 3)], recv_sem.at[0, q])
        pltpu.make_async_copy(b1.at[q, :, 0], b1.at[q, :, 0], own_sem.at[q]).wait()
        four(b1, q, turn_y)
        for d in (1, 3, 2):
            to = (y + d) % 4
            send(b1.at[q, :, to], b2.at[q, :, y], 1, recv_sem.at[1, q], device(z, to, x, c))
        for p in range(2):
            b2[q, p, y] = b1[q, p, y]

    def step_y(q):
        landed(b2.at[q, :, pl.ds(0, 3)], recv_sem.at[1, q])
        four(b2, q, turn_x)
        for d, t in ((1, 0), (3, 0), (2, 0), (1, 1), (3, 1), (2, 1), (0, 1)):
            tx, tc = (x + d) % 4, (c + t) % 2
            send(
                b2.at[q, :, tx, :, pl.ds(pl.multiple_of(tc * 16, 16), 16)],
                b3.at[q, :, x * 2 + c],
                2, recv_sem.at[2, q], device(z, y, tx, tc),
            )
        for p in range(2):
            b3[q, p, x * 2 + c] = b2[q, p, x, :, pl.ds(pl.multiple_of(c * 16, 16), 16)]

    def step_x(q):
        landed(b3.at[q, :, pl.ds(0, 7)], recv_sem.at[2, q])

        @pl.loop(0, 8)
        def _(i):
            v = dft8([(b3[q, 0, k, i], b3[q, 1, k, i]) for k in range(8)])
            for k in range(8):
                b3[q, 0, k, i] = v[k][0]
                b3[q, 1, k, i] = v[k][1]

        for d, t in ((1, 0), (3, 0), (2, 0), (1, 1), (3, 1), (2, 1), (0, 1)):
            tz, tc = (z + d) % 4, (c + t) % 2
            send(
                b3.at[q, :, tz * 2 + tc],
                b4.at[q, :, :, z * 2 + c],
                3, recv_sem.at[3, q], device(tz, y, x, tc),
            )
        for p in range(2):
            b4[q, p, :, z * 2 + c] = b3[q, p, z * 2 + c]

    def step_local(q):
        landed(b4.at[q, :, :, pl.ds(0, 7)], recv_sem.at[3, q])

        @pl.loop(0, 4)
        def _(pair):
            block = jnp.concatenate(
                [
                    jnp.concatenate([b4[q, p, pair * 2 + t].reshape(128, 128) for t in range(2)], axis=1)
                    for p in range(2)
                ],
                axis=0,
            )
            hi, lo = split(block)
            result = jnp.dot(g_hi[...], hi, preferred_element_type=F32)
            result += jnp.dot(g_hi[...], lo, preferred_element_type=F32)
            result += jnp.dot(g_lo[...], hi, preferred_element_type=F32)
            for t in range(2):
                f = (pair * 2 + t) * 4 + q
                value = (result[:128, t * 128 : t * 128 + 128], result[128:, t * 128 : t * 128 + 128])
                value = times(value, (turn[0, f], turn[1, f]))
                for p in range(2):
                    b4[q, p, pair * 2 + t] = value[p].reshape(8, 16, 128)

        @pl.loop(0, 8)
        def _(g):
            v = dft8([(b4[q, 0, i, g], b4[q, 1, i, g]) for i in range(8)])
            for i in range(8):
                b4[q, 0, i, g] = v[i][0]
                b4[q, 1, i, g] = v[i][1]

    def finish(j):
        roots = [
            (math.cos(-2 * math.pi * q * j / 32), math.sin(-2 * math.pi * q * j / 32)) for q in range(4)
        ]

        @pl.loop(0, 8)
        def _(g):
            v = [(b4[q, 0, j, g], b4[q, 1, j, g]) for q in range(4)]
            if j:
                v = [v[0]] + [times(v[q], roots[q]) for q in range(1, 4)]
            v = dft4(v)
            where = pl.ds(pl.multiple_of(g * 16, 16), 16)
            for m in range(4):
                row = j + 8 * m
                w = times(v[m], (lanes[0, row : row + 1], lanes[1, row : row + 1]))
                for p in range(2):
                    hi, lo = split(w[p])
                    z_hi[m, where, p * 128 : (p + 1) * 128] = hi
                    z_lo[m, where, p * 128 : (p + 1) * 128] = lo

        flat = p0.at[j].reshape(1024, 128)
        dims = (((1,), (1,)), ((), ()))
        for pair in range(2):
            hi = z_hi[pair * 2 : pair * 2 + 2].reshape(256, 256)
            lo = z_lo[pair * 2 : pair * 2 + 2].reshape(256, 256)
            result = lax.dot_general(h_hi[...], hi, dims, preferred_element_type=F32)
            result += lax.dot_general(h_hi[...], lo, dims, preferred_element_type=F32)
            result += lax.dot_general(h_lo[...], hi, dims, preferred_element_type=F32)
            for p in range(2):
                for t in range(2):
                    flat[pl.ds(p * 4 + pair * 2 + t, 128, stride=8), :] = result[
                        p * 128 : p * 128 + 128, t * 128 : t * 128 + 128
                    ]

    buffers = (p0, p1, p2, p3)

    def leave(j, stage):
        src, dst, sem = buffers[stage].at[j], buffers[stage + 1].at[j], last_sem.at[stage, j]
        axis = ORDERS[j][stage]
        if axis == "z":
            for d in (1, 3, 2):
                to = (z + d) % 4
                send(src.at[to], dst.at[z], 4 + stage, sem, device(to, y, x, c))
            dst[z] = src[z]
        elif axis == "y":
            for d in (1, 3, 2):
                to = (y + d) % 4
                send(src.at[:, :, :, to], dst.at[:, :, :, y], 4 + stage, sem, device(z, to, x, c))
            dst[:, :, :, y] = src[:, :, :, y]
        else:
            for d, t in ((1, 0), (3, 0), (2, 0), (1, 1), (3, 1), (2, 1), (0, 1)):
                tx, tc = (x + d) % 4, (c + t) % 2
                send(src.at[:, tc, tx], dst.at[:, c, x], 4 + stage, sem, device(z, y, tx, tc))
            dst[:, c, x] = src[:, c, x]

    def arrive(j, stage):
        dst, sem = buffers[stage + 1].at[j], last_sem.at[stage, j]
        axis = ORDERS[j][stage]
        if axis == "z":
            landed(dst.at[pl.ds(0, 3)], sem)
        elif axis == "y":
            landed(dst.at[:, :, :, pl.ds(0, 3)], sem)
        else:
            flat = buffers[stage + 1].at[j].reshape(128, 8, 128)
            landed(flat.at[pl.ds(0, 112)], sem)

    def write(j):
        flat = p3.at[j].reshape(1024, 128)
        for p in range(2):
            for m in range(4):
                row = (j + 8 * m) * 128
                out[p, row : row + 128] = flat[pl.ds(p * 4 + m, 128, stride=8), :].T
                pltpu.make_async_copy(
                    out.at[p, pl.ds(row, 128)], outputs[p].at[pl.ds(row, 128)], out_sem
                ).start()

    step_z(0)
    step_z(1)
    step_y(0)
    step_z(2)
    step_y(1)
    step_x(0)
    step_z(3)
    step_y(2)
    step_x(1)
    step_y(3)
    step_x(2)
    step_local(0)
    step_x(3)
    step_local(1)
    step_local(2)
    step_local(3)

    for j in range(8):
        finish(j)
        leave(j, 0)
    for j, stage in (
        (0, 0), (1, 0), (2, 0), (3, 0), (4, 0), (5, 0), (6, 0), (7, 0), (1, 1), (0, 1), (2, 1), (4, 1),
        (3, 1), (5, 1), (7, 1), (6, 1), (1, 2), (0, 2), (2, 2), (4, 2), (3, 2), (5, 2), (7, 2), (6, 2),
    ):
        arrive(j, stage)
        if stage < 2:
            leave(j, stage + 1)
        else:
            write(j)

    for p in range(2):
        pltpu.make_async_copy(out.at[p], outputs[p], out_sem).wait()

    def sent(ref, stage):
        pltpu.make_async_remote_copy(
            src_ref=ref, dst_ref=ref, send_sem=send_sem.at[stage], recv_sem=send_sem.at[stage],
            device_id=(me,), device_id_type=MESH,
        ).wait_send()

    sent(b1.at[pl.ds(0, 3)], 0)
    sent(b2.at[pl.ds(0, 3)], 1)
    sent(b3.at[:, :, pl.ds(0, 7)], 2)
    sent(b3.at[:, :, pl.ds(0, 7)], 3)
    for stage in range(3):
        eighths = sum(7 if order[stage] == "x" else 6 for order in ORDERS)
        sent(p0.reshape(64, 128, 128).at[pl.ds(0, eighths)], 4 + stage)


def body(signal_real, signal_imag):
    shape = (4, 32, 32, 1, 128)
    block = (8, 4, 2, 4, 4, 8, 128)
    out_re, out_im = pl.pallas_call(
        kernel,
        out_shape=[jax.ShapeDtypeStruct((4096, 128), F32)] * 2,
        in_specs=[pl.BlockSpec(memory_space=pl.ANY)] * 2,
        out_specs=[pl.BlockSpec(memory_space=pl.ANY)] * 2,
        scratch_shapes=[
            pltpu.VMEM((4, 2, 4, 8, 32, 128), F32),
            pltpu.VMEM((4, 2, 4, 8, 32, 128), F32),
            pltpu.VMEM((4, 2, 8, 8, 16, 128), F32),
            pltpu.VMEM((4, 2, 8, 8, 16, 128), F32),
            pltpu.VMEM(block, F32),
            pltpu.VMEM(block, F32),
            pltpu.VMEM(block, F32),
            pltpu.VMEM(block, F32),
            pltpu.VMEM((2, 32, 128, 128), F32),
            pltpu.VMEM((2, 4096, 128), F32),
            pltpu.VMEM((4, 128, 256), BF16),
            pltpu.VMEM((4, 128, 256), BF16),
            pltpu.VMEM((256, 256), BF16),
            pltpu.VMEM((256, 256), BF16),
            pltpu.VMEM((256, 256), BF16),
            pltpu.VMEM((256, 256), BF16),
            pltpu.VMEM((2, 32, 128), F32),
            pltpu.SemaphoreType.DMA((4,)),
            pltpu.SemaphoreType.DMA((7,)),
            pltpu.SemaphoreType.DMA((4, 4)),
            pltpu.SemaphoreType.DMA((3, 8)),
            pltpu.SemaphoreType.DMA,
        ],
        compiler_params=pltpu.CompilerParams(collective_id=0, has_side_effects=True, vmem_limit_bytes=60 * 2**20),
    )(signal_real.reshape(shape), signal_imag.reshape(shape))
    return out_re.reshape(-1), out_im.reshape(-1)


def solution(mesh):
    return jax.shard_map(
        body, mesh=mesh, in_specs=(P("pa"), P("pa")), out_specs=(P("pa"), P("pa")), check_vma=False
    )
```

```python
import math

import jax
import jax.numpy as jnp
from jax import lax
from jax.experimental import pallas as pl
from jax.experimental.pallas import tpu as pltpu
from jax.sharding import PartitionSpec as P

MESH = pl.DeviceIdType.MESH
F32 = jnp.float32
BF16 = jnp.bfloat16
ROOT_HALF = math.sqrt(0.5)
ORDERS = ("zxy", "xyz", "yzx", "zxy", "xyz", "yzx", "zxy", "xyz")


def device(z, y, x, c):
    return ((z * 4 + y) * 4 + x) * 2 + c


def unit_root(phase, bits):
    phase = phase & ((1 << bits) - 1)
    quarter = (phase + (1 << (bits - 3))) >> (bits - 2)
    angle = (phase - (quarter << (bits - 2))).astype(F32) * (2.0 * math.pi / (1 << bits))
    square = angle * angle
    sine = angle * (1.0 + square * (-1 / 6 + square * (1 / 120 + square * (-1 / 5040 + square * (1 / 362880)))))
    cosine = 1.0 + square * (-1 / 2 + square * (1 / 24 + square * (-1 / 720 + square * (1 / 40320))))
    odd = (quarter & 1) == 1
    real = jnp.where(odd, sine, cosine)
    imag = jnp.where(odd, cosine, sine)
    real = jnp.where(((quarter + 1) & 2) == 2, -real, real)
    imag = jnp.where((quarter & 2) == 2, imag, -imag)
    return real, imag


def times(value, factor):
    (a, b), (c, d) = value, factor
    return a * c - b * d, a * d + b * c


def plus(a, b):
    return a[0] + b[0], a[1] + b[1]


def minus(a, b):
    return a[0] - b[0], a[1] - b[1]


def dft4(v):
    s, d = plus(v[0], v[2]), minus(v[0], v[2])
    t, u = plus(v[1], v[3]), minus(v[1], v[3])
    return [plus(s, t), (d[0] + u[1], d[1] - u[0]), minus(s, t), (d[0] - u[1], d[1] + u[0])]


def dft8(v):
    even, odd = dft4(v[0::2]), dft4(v[1::2])
    turned = [
        odd[0],
        ((odd[1][0] + odd[1][1]) * ROOT_HALF, (odd[1][1] - odd[1][0]) * ROOT_HALF),
        (odd[2][1], -odd[2][0]),
        ((odd[3][1] - odd[3][0]) * ROOT_HALF, (odd[3][0] + odd[3][1]) * -ROOT_HALF),
    ]
    return [plus(e, t) for e, t in zip(even, turned)] + [minus(e, t) for e, t in zip(even, turned)]


def split(value):
    high = value.astype(BF16)
    return high, (value - high.astype(F32)).astype(BF16)


def kernel(
    re_hbm, im_hbm, out_re, out_im,
    b1, b2, b3, b4, p0, p1, p2, p3, turn, z_hi, z_lo, g_hi, g_lo, h_hi, h_lo, lanes,
    own_sem, send_sem, recv_sem, last_sem,
):
    me = lax.axis_index("pa")
    z, y, x, c = me // 32, (me // 8) % 4, (me // 2) % 4, me % 2
    inputs, outputs = (re_hbm, im_hbm), (out_re, out_im)

    barrier = pltpu.get_barrier_semaphore()
    peers = [device(z, (y + d) % 4, x, c) for d in (1, 2, 3)]
    peers += [device(z, y, (x + d) % 4, (c + t) % 2) for d in range(4) for t in range(2) if d + t]
    peers += [device((z + d) % 4, y, x, (c + t) % 2) for d in (1, 2, 3) for t in range(2)]
    for peer in peers:
        pl.semaphore_signal(barrier, inc=1, device_id=(peer,), device_id_type=MESH)
    pl.semaphore_wait(barrier, len(peers))

    def send(src, dst, stage, sem, peer):
        pltpu.make_async_remote_copy(
            src_ref=src, dst_ref=dst, send_sem=send_sem.at[stage], recv_sem=sem, device_id=(peer,), device_id_type=MESH
        ).start()

    def landed(ref, sem):
        pltpu.make_async_remote_copy(
            src_ref=ref, dst_ref=ref, send_sem=sem, recv_sem=sem, device_id=(me,), device_id_type=MESH
        ).wait_recv()

    for q in range(4):
        for part in range(2):

            @pl.loop(0, 8)
            def _(i):
                for d in (1, 3, 2):
                    to = (z + d) % 4
                    send(
                        inputs[part].at[to, :, i * 4 + q, 0],
                        b1.at[q, part, z, i],
                        0, recv_sem.at[0, q], device(to, y, x, c),
                    )
                pltpu.make_async_copy(
                    inputs[part].at[z, :, i * 4 + q, 0], b1.at[q, part, z, i], own_sem.at[q]
                ).start()

    s = z * 32 + c * 16 + x * 4 + y
    rows = lax.broadcasted_iota(jnp.int32, (128, 128), 0)
    cols = lax.broadcasted_iota(jnp.int32, (128, 128), 1)

    def matrix(phase, bits, scale, high, low):
        real, imag = unit_root(phase, bits)
        real, imag = real * scale, imag * scale
        for r, k, block in ((0, 0, real), (0, 1, -imag), (1, 0, imag), (1, 1, real)):
            hi, lo = split(block)
            high[r * 128 : (r + 1) * 128, k * 128 : (k + 1) * 128] = hi
            low[r * 128 : (r + 1) * 128, k * 128 : (k + 1) * 128] = lo

    matrix((rows * 128 + s) * cols, 14, 1.0, g_hi, g_lo)
    target = (rows & 96) + (rows & 3) * 8 + ((rows >> 2) & 3) * 2 + ((rows >> 4) & 1)
    matrix(target * cols, 7, 1.0 / 8192.0, h_hi, h_lo)
    lane_rows = lax.broadcasted_iota(jnp.int32, (32, 128), 0)
    lane_cols = lax.broadcasted_iota(jnp.int32, (32, 128), 1)
    lanes[0], lanes[1] = unit_root(lane_rows * lane_cols, 12)

    @pl.loop(0, 32)
    def _(f):
        real, imag = unit_root((rows * 128 + s) * (cols + f * 128), 26)
        turn[0, f] = real
        turn[1, f] = imag

    def scalar_root(phase, bits):
        return unit_root(jnp.full((8, 128), 1, jnp.int32) * phase, bits)

    turn_y = [scalar_root(k * y, 4) for k in range(4)]
    turn_x = [scalar_root((4 * k + y) * (2 * x + c), 7) for k in range(4)]

    def four(buf, q, factors):
        @pl.loop(0, 8)
        def _(i):
            v = [tuple(buf[q, p, k, i].reshape(4, 8, 128) for p in range(2)) for k in range(4)]
            v = [times(o, (w[0][None], w[1][None])) for o, w in zip(dft4(v), factors)]
            for k in range(4):
                for p in range(2):
                    buf[q, p, k, i] = v[k][p].reshape(32, 128)

    def step_z(q):
        landed(b1.at[q, :, pl.ds(0, 3)], recv_sem.at[0, q])
        pltpu.make_async_copy(b1.at[q, :, 0], b1.at[q, :, 0], own_sem.at[q]).wait()
        four(b1, q, turn_y)
        for d in (1, 3, 2):
            to = (y + d) % 4
            send(b1.at[q, :, to], b2.at[q, :, y], 1, recv_sem.at[1, q], device(z, to, x, c))
        for p in range(2):
            b2[q, p, y] = b1[q, p, y]

    def step_y(q):
        landed(b2.at[q, :, pl.ds(0, 3)], recv_sem.at[1, q])
        four(b2, q, turn_x)
        for d, t in ((1, 0), (3, 0), (2, 0), (1, 1), (3, 1), (2, 1), (0, 1)):
            tx, tc = (x + d) % 4, (c + t) % 2
            send(
                b2.at[q, :, tx, :, pl.ds(pl.multiple_of(tc * 16, 16), 16)],
                b3.at[q, :, x * 2 + c],
                2, recv_sem.at[2, q], device(z, y, tx, tc),
            )
        for p in range(2):
            b3[q, p, x * 2 + c] = b2[q, p, x, :, pl.ds(pl.multiple_of(c * 16, 16), 16)]

    def step_x(q):
        landed(b3.at[q, :, pl.ds(0, 7)], recv_sem.at[2, q])

        @pl.loop(0, 8)
        def _(i):
            v = dft8([(b3[q, 0, k, i], b3[q, 1, k, i]) for k in range(8)])
            for k in range(8):
                b3[q, 0, k, i] = v[k][0]
                b3[q, 1, k, i] = v[k][1]

        for d, t in ((1, 0), (3, 0), (2, 0), (1, 1), (3, 1), (2, 1), (0, 1)):
            tz, tc = (z + d) % 4, (c + t) % 2
            send(
                b3.at[q, :, tz * 2 + tc],
                b4.at[q, :, :, z * 2 + c],
                3, recv_sem.at[3, q], device(tz, y, x, tc),
            )
        for p in range(2):
            b4[q, p, :, z * 2 + c] = b3[q, p, z * 2 + c]

    def step_local(q):
        landed(b4.at[q, :, :, pl.ds(0, 7)], recv_sem.at[3, q])

        @pl.loop(0, 4)
        def _(pair):
            block = jnp.concatenate(
                [
                    jnp.concatenate([b4[q, p, pair * 2 + t].reshape(128, 128) for t in range(2)], axis=1)
                    for p in range(2)
                ],
                axis=0,
            )
            hi, lo = split(block)
            result = jnp.dot(g_hi[...], hi, preferred_element_type=F32)
            result += jnp.dot(g_hi[...], lo, preferred_element_type=F32)
            result += jnp.dot(g_lo[...], hi, preferred_element_type=F32)
            for t in range(2):
                f = (pair * 2 + t) * 4 + q
                value = (result[:128, t * 128 : t * 128 + 128], result[128:, t * 128 : t * 128 + 128])
                value = times(value, (turn[0, f], turn[1, f]))
                for p in range(2):
                    b4[q, p, pair * 2 + t] = value[p].reshape(8, 16, 128)

        @pl.loop(0, 8)
        def _(g):
            v = dft8([(b4[q, 0, i, g], b4[q, 1, i, g]) for i in range(8)])
            for i in range(8):
                b4[q, 0, i, g] = v[i][0]
                b4[q, 1, i, g] = v[i][1]

    def finish(j):
        roots = [
            (math.cos(-2 * math.pi * q * j / 32), math.sin(-2 * math.pi * q * j / 32)) for q in range(4)
        ]

        @pl.loop(0, 8)
        def _(g):
            v = [(b4[q, 0, j, g], b4[q, 1, j, g]) for q in range(4)]
            if j:
                v = [v[0]] + [times(v[q], roots[q]) for q in range(1, 4)]
            v = dft4(v)
            where = pl.ds(pl.multiple_of(g * 16, 16), 16)
            for m in range(4):
                row = j + 8 * m
                w = times(v[m], (lanes[0, row : row + 1], lanes[1, row : row + 1]))
                for p in range(2):
                    hi, lo = split(w[p])
                    z_hi[m, where, p * 128 : (p + 1) * 128] = hi
                    z_lo[m, where, p * 128 : (p + 1) * 128] = lo

        flat = p0.at[j].reshape(1024, 128)
        dims = (((1,), (1,)), ((), ()))
        for pair in range(2):
            hi = z_hi[pair * 2 : pair * 2 + 2].reshape(256, 256)
            lo = z_lo[pair * 2 : pair * 2 + 2].reshape(256, 256)
            result = lax.dot_general(h_hi[...], hi, dims, preferred_element_type=F32)
            result += lax.dot_general(h_hi[...], lo, dims, preferred_element_type=F32)
            result += lax.dot_general(h_lo[...], hi, dims, preferred_element_type=F32)
            for p in range(2):
                for t in range(2):
                    flat[pl.ds(p * 4 + pair * 2 + t, 128, stride=8), :] = result[
                        p * 128 : p * 128 + 128, t * 128 : t * 128 + 128
                    ]

    buffers = (p0, p1, p2, p3)

    def leave(j, stage):
        src, dst, sem = buffers[stage].at[j], buffers[stage + 1].at[j], last_sem.at[stage, j]
        axis = ORDERS[j][stage]
        if axis == "z":
            for d in (1, 3, 2):
                to = (z + d) % 4
                send(src.at[to], dst.at[z], 4 + stage, sem, device(to, y, x, c))
            dst[z] = src[z]
        elif axis == "y":
            for d in (1, 3, 2):
                to = (y + d) % 4
                send(src.at[:, :, :, to], dst.at[:, :, :, y], 4 + stage, sem, device(z, to, x, c))
            dst[:, :, :, y] = src[:, :, :, y]
        else:
            for d, t in ((1, 0), (3, 0), (2, 0), (1, 1), (3, 1), (2, 1), (0, 1)):
                tx, tc = (x + d) % 4, (c + t) % 2
                send(src.at[:, tc, tx], dst.at[:, c, x], 4 + stage, sem, device(z, y, tx, tc))
            dst[:, c, x] = src[:, c, x]

    def arrive(j, stage):
        dst, sem = buffers[stage + 1].at[j], last_sem.at[stage, j]
        axis = ORDERS[j][stage]
        if axis == "z":
            landed(dst.at[pl.ds(0, 3)], sem)
        elif axis == "y":
            landed(dst.at[:, :, :, pl.ds(0, 3)], sem)
        else:
            flat = buffers[stage + 1].at[j].reshape(128, 8, 128)
            landed(flat.at[pl.ds(0, 112)], sem)

    def write(j):
        flat = p3.at[j].reshape(1024, 128)
        for p in range(2):
            for m in range(4):
                row = (j + 8 * m) * 128
                outputs[p][row : row + 128] = flat[pl.ds(p * 4 + m, 128, stride=8), :].T

    step_z(0)
    step_z(1)
    step_y(0)
    step_z(2)
    step_y(1)
    step_x(0)
    step_z(3)
    step_y(2)
    step_x(1)
    step_y(3)
    step_x(2)
    step_local(0)
    step_x(3)
    step_local(1)
    step_local(2)
    step_local(3)

    for j in range(8):
        finish(j)
        leave(j, 0)
    for j, stage in (
        (0, 0), (1, 0), (2, 0), (3, 0), (4, 0), (5, 0), (6, 0), (7, 0), (1, 1), (0, 1), (2, 1), (4, 1),
        (3, 1), (5, 1), (7, 1), (6, 1), (1, 2), (0, 2), (2, 2), (4, 2), (3, 2), (5, 2), (7, 2), (6, 2),
    ):
        arrive(j, stage)
        if stage < 2:
            leave(j, stage + 1)
        else:
            write(j)

    def sent(ref, stage):
        pltpu.make_async_remote_copy(
            src_ref=ref, dst_ref=ref, send_sem=send_sem.at[stage], recv_sem=send_sem.at[stage],
            device_id=(me,), device_id_type=MESH,
        ).wait_send()

    sent(b1.at[pl.ds(0, 3)], 0)
    sent(b2.at[pl.ds(0, 3)], 1)
    sent(b3.at[:, :, pl.ds(0, 7)], 2)
    sent(b3.at[:, :, pl.ds(0, 7)], 3)
    for stage in range(3):
        eighths = sum(7 if order[stage] == "x" else 6 for order in ORDERS)
        sent(p0.reshape(64, 128, 128).at[pl.ds(0, eighths)], 4 + stage)


def store(re_ref, im_ref, out_re, out_im, sems):
    copies = [
        pltpu.make_async_copy(src.at[pl.ds(k * 512, 512)], dst.at[pl.ds(k * 512, 512)], sems.at[p, k])
        for k in range(8)
        for p, (src, dst) in enumerate(((re_ref, out_re), (im_ref, out_im)))
    ]
    for copy in copies:
        copy.start()
    for copy in copies:
        copy.wait()


def body(signal_real, signal_imag):
    shape = (4, 32, 32, 1, 128)
    block = (8, 4, 2, 4, 4, 8, 128)
    spectrum = pl.pallas_call(
        kernel,
        out_shape=[pltpu.VMEM((4096, 128), F32)] * 2,
        in_specs=[pl.BlockSpec(memory_space=pl.ANY)] * 2,
        out_specs=[pl.BlockSpec(memory_space=pltpu.VMEM)] * 2,
        scratch_shapes=[
            pltpu.VMEM((4, 2, 4, 8, 32, 128), F32),
            pltpu.VMEM((4, 2, 4, 8, 32, 128), F32),
            pltpu.VMEM((4, 2, 8, 8, 16, 128), F32),
            pltpu.VMEM((4, 2, 8, 8, 16, 128), F32),
            pltpu.VMEM(block, F32),
            pltpu.VMEM(block, F32),
            pltpu.VMEM(block, F32),
            pltpu.VMEM(block, F32),
            pltpu.VMEM((2, 32, 128, 128), F32),
            pltpu.VMEM((4, 128, 256), BF16),
            pltpu.VMEM((4, 128, 256), BF16),
            pltpu.VMEM((256, 256), BF16),
            pltpu.VMEM((256, 256), BF16),
            pltpu.VMEM((256, 256), BF16),
            pltpu.VMEM((256, 256), BF16),
            pltpu.VMEM((2, 32, 128), F32),
            pltpu.SemaphoreType.DMA((4,)),
            pltpu.SemaphoreType.DMA((7,)),
            pltpu.SemaphoreType.DMA((4, 4)),
            pltpu.SemaphoreType.DMA((3, 8)),
        ],
        compiler_params=pltpu.CompilerParams(collective_id=0, has_side_effects=True, vmem_limit_bytes=48 * 2**20),
    )(signal_real.reshape(shape), signal_imag.reshape(shape))
    out_re, out_im = pl.pallas_call(
        store,
        out_shape=[jax.ShapeDtypeStruct((4096, 128), F32)] * 2,
        in_specs=[pl.BlockSpec(memory_space=pltpu.VMEM)] * 2,
        out_specs=[pl.BlockSpec(memory_space=pl.ANY)] * 2,
        scratch_shapes=[pltpu.SemaphoreType.DMA((2, 8))],
        compiler_params=pltpu.CompilerParams(vmem_limit_bytes=8 * 2**20),
    )(*spectrum)
    return out_re.reshape(-1), out_im.reshape(-1)


def solution(mesh):
    return jax.shard_map(
        body, mesh=mesh, in_specs=(P("pa"), P("pa")), out_specs=(P("pa"), P("pa")), check_vma=False
    )
```

```python
import math

import jax
import jax.numpy as jnp
from jax import lax
from jax.experimental import pallas as pl
from jax.experimental.pallas import tpu as pltpu
from jax.sharding import PartitionSpec as P

MESH = pl.DeviceIdType.MESH
F32 = jnp.float32
BF16 = jnp.bfloat16
ROOT_HALF = math.sqrt(0.5)
ORDERS = ('yxz', 'zyx', 'xzy', 'zyx', 'xzy', 'xyz', 'yxz', 'zyx')


def device(z, y, x, c):
    return ((z * 4 + y) * 4 + x) * 2 + c


def unit_root(phase, bits):
    phase = phase & ((1 << bits) - 1)
    quarter = (phase + (1 << (bits - 3))) >> (bits - 2)
    angle = (phase - (quarter << (bits - 2))).astype(F32) * (2.0 * math.pi / (1 << bits))
    square = angle * angle
    sine = angle * (1.0 + square * (-1 / 6 + square * (1 / 120 + square * (-1 / 5040 + square * (1 / 362880)))))
    cosine = 1.0 + square * (-1 / 2 + square * (1 / 24 + square * (-1 / 720 + square * (1 / 40320))))
    odd = (quarter & 1) == 1
    real = jnp.where(odd, sine, cosine)
    imag = jnp.where(odd, cosine, sine)
    real = jnp.where(((quarter + 1) & 2) == 2, -real, real)
    imag = jnp.where((quarter & 2) == 2, imag, -imag)
    return real, imag


def times(value, factor):
    (a, b), (c, d) = value, factor
    return a * c - b * d, a * d + b * c


def plus(a, b):
    return a[0] + b[0], a[1] + b[1]


def minus(a, b):
    return a[0] - b[0], a[1] - b[1]


def dft4(v):
    s, d = plus(v[0], v[2]), minus(v[0], v[2])
    t, u = plus(v[1], v[3]), minus(v[1], v[3])
    return [plus(s, t), (d[0] + u[1], d[1] - u[0]), minus(s, t), (d[0] - u[1], d[1] + u[0])]


def dft8(v):
    even, odd = dft4(v[0::2]), dft4(v[1::2])
    turned = [
        odd[0],
        ((odd[1][0] + odd[1][1]) * ROOT_HALF, (odd[1][1] - odd[1][0]) * ROOT_HALF),
        (odd[2][1], -odd[2][0]),
        ((odd[3][1] - odd[3][0]) * ROOT_HALF, (odd[3][0] + odd[3][1]) * -ROOT_HALF),
    ]
    return [plus(e, t) for e, t in zip(even, turned)] + [minus(e, t) for e, t in zip(even, turned)]


def split(value):
    high = value.astype(BF16)
    return high, (value - high.astype(F32)).astype(BF16)


def kernel(
    re_hbm, im_hbm, out_re, out_im,
    b1, b2, b3, b4, p0, p1, p2, p3, turn, z_hi, z_lo, g, h, lanes,
    own_sem, send_sem, recv_sem, last_sem,
):
    me = lax.axis_index("pa")
    z, y, x, c = me // 32, (me // 8) % 4, (me // 2) % 4, me % 2
    inputs, outputs = (re_hbm, im_hbm), (out_re, out_im)

    barrier = pltpu.get_barrier_semaphore()
    peers = [device(z, (y + d) % 4, x, c) for d in (1, 2, 3)]
    peers += [device(z, y, (x + d) % 4, (c + t) % 2) for d in range(4) for t in range(2) if d + t]
    peers += [device((z + d) % 4, y, x, (c + t) % 2) for d in (1, 2, 3) for t in range(2)]
    for peer in peers:
        pl.semaphore_signal(barrier, inc=1, device_id=(peer,), device_id_type=MESH)
    pl.semaphore_wait(barrier, len(peers))

    def send(src, dst, stage, sem, peer):
        pltpu.make_async_remote_copy(
            src_ref=src, dst_ref=dst, send_sem=send_sem.at[stage], recv_sem=sem, device_id=(peer,), device_id_type=MESH
        ).start()

    def landed(ref, sem):
        pltpu.make_async_remote_copy(
            src_ref=ref, dst_ref=ref, send_sem=sem, recv_sem=sem, device_id=(me,), device_id_type=MESH
        ).wait_recv()

    for q in range(4):
        for part in range(2):

            @pl.loop(0, 8)
            def _(i):
                for d in (2, 1, 3):
                    to = (z + d) % 4
                    send(
                        inputs[part].at[to, :, i * 4 + q, 0],
                        b1.at[q, part, z, i],
                        0, recv_sem.at[0, q], device(to, y, x, c),
                    )
                pltpu.make_async_copy(
                    inputs[part].at[z, :, i * 4 + q, 0], b1.at[q, part, z, i], own_sem.at[q]
                ).start()

    s = z * 32 + c * 16 + x * 4 + y
    rows = lax.broadcasted_iota(jnp.int32, (128, 128), 0)
    cols = lax.broadcasted_iota(jnp.int32, (128, 128), 1)

    def matrix(phase, bits, scale, table):
        real, imag = unit_root(phase, bits)
        real, imag = real * scale, imag * scale
        for r, k, block in ((0, 0, real), (0, 1, -imag), (1, 0, imag), (1, 1, real)):
            hi, lo = split(block)
            table[r * 128 : r * 128 + 128, k * 128 : k * 128 + 128] = hi
            table[r * 128 + 256 : r * 128 + 384, k * 128 : k * 128 + 128] = lo

    matrix((rows * 128 + s) * cols, 14, 1.0, g)
    target = (rows & 96) + (rows & 3) * 8 + ((rows >> 2) & 3) * 2 + ((rows >> 4) & 1)
    matrix(target * cols, 7, 1.0 / 8192.0, h)
    lane_rows = lax.broadcasted_iota(jnp.int32, (32, 128), 0)
    lane_cols = lax.broadcasted_iota(jnp.int32, (32, 128), 1)
    lanes[0], lanes[1] = unit_root(lane_rows * lane_cols, 12)

    @pl.loop(0, 32)
    def _(f):
        real, imag = unit_root((rows * 128 + s) * (cols + f * 128), 26)
        turn[0, f] = real
        turn[1, f] = imag

    def scalar_root(phase, bits):
        return unit_root(jnp.full((8, 128), 1, jnp.int32) * phase, bits)

    turn_y = [scalar_root(k * y, 4) for k in range(4)]
    turn_x = [scalar_root((4 * k + y) * (2 * x + c), 7) for k in range(4)]

    def four(buf, q, factors):
        @pl.loop(0, 8)
        def _(i):
            v = [tuple(buf[q, p, k, i].reshape(4, 8, 128) for p in range(2)) for k in range(4)]
            v = [times(o, (w[0][None], w[1][None])) for o, w in zip(dft4(v), factors)]
            for k in range(4):
                for p in range(2):
                    buf[q, p, k, i] = v[k][p].reshape(32, 128)

    def step_z(q):
        landed(b1.at[q, :, pl.ds(0, 3)], recv_sem.at[0, q])
        pltpu.make_async_copy(b1.at[q, :, 0], b1.at[q, :, 0], own_sem.at[q]).wait()
        four(b1, q, turn_y)
        for d in (2, 1, 3):
            to = (y + d) % 4
            send(b1.at[q, :, to], b2.at[q, :, y], 1, recv_sem.at[1, q], device(z, to, x, c))
        for p in range(2):
            b2[q, p, y] = b1[q, p, y]

    def step_y(q):
        landed(b2.at[q, :, pl.ds(0, 3)], recv_sem.at[1, q])
        four(b2, q, turn_x)
        for d, t in ((2, 1), (2, 0), (1, 1), (3, 1), (1, 0), (3, 0), (0, 1)):
            tx, tc = (x + d) % 4, (c + t) % 2
            send(
                b2.at[q, :, tx, :, pl.ds(pl.multiple_of(tc * 16, 16), 16)],
                b3.at[q, :, x * 2 + c],
                2, recv_sem.at[2, q], device(z, y, tx, tc),
            )
        for p in range(2):
            b3[q, p, x * 2 + c] = b2[q, p, x, :, pl.ds(pl.multiple_of(c * 16, 16), 16)]

    def step_x(q):
        landed(b3.at[q, :, pl.ds(0, 7)], recv_sem.at[2, q])

        @pl.loop(0, 8)
        def _(i):
            v = dft8([(b3[q, 0, k, i], b3[q, 1, k, i]) for k in range(8)])
            for k in range(8):
                b3[q, 0, k, i] = v[k][0]
                b3[q, 1, k, i] = v[k][1]

        def leave_x(tz, tc):
            send(
                b3.at[q, :, tz * 2 + tc],
                b4.at[q, :, :, z * 2 + c],
                3, recv_sem.at[3, q], device(tz, y, x, tc),
            )

        leave_x(z, 1 - c)
        for tc in range(2):
            for d in (2, 1, 3):
                leave_x((z + d) % 4, tc)
        for p in range(2):
            b4[q, p, :, z * 2 + c] = b3[q, p, z * 2 + c]

    def step_local(q):
        landed(b4.at[q, :, :, pl.ds(0, 7)], recv_sem.at[3, q])

        @pl.loop(0, 4, unroll=True)
        def _(pair):
            block = jnp.concatenate(
                [
                    jnp.concatenate([b4[q, p, pair * 2 + t].reshape(128, 128) for t in range(2)], axis=1)
                    for p in range(2)
                ],
                axis=0,
            )
            hi, lo = split(block)
            both = jnp.dot(g[...], hi, preferred_element_type=F32)
            result = both[:256] + both[256:] + jnp.dot(g[:256], lo, preferred_element_type=F32)
            for t in range(2):
                f = (pair * 2 + t) * 4 + q
                value = (result[:128, t * 128 : t * 128 + 128], result[128:, t * 128 : t * 128 + 128])
                value = times(value, (turn[0, f], turn[1, f]))
                for p in range(2):
                    b4[q, p, pair * 2 + t] = value[p].reshape(8, 16, 128)

        @pl.loop(0, 8, unroll=True)
        def _(g):
            v = dft8([(b4[q, 0, i, g], b4[q, 1, i, g]) for i in range(8)])
            for i in range(8):
                b4[q, 0, i, g] = v[i][0]
                b4[q, 1, i, g] = v[i][1]

    def finish(j):
        roots = [
            (math.cos(-2 * math.pi * q * j / 32), math.sin(-2 * math.pi * q * j / 32)) for q in range(4)
        ]

        @pl.loop(0, 8, unroll=True)
        def _(g):
            v = [(b4[q, 0, j, g], b4[q, 1, j, g]) for q in range(4)]
            if j:
                v = [v[0]] + [times(v[q], roots[q]) for q in range(1, 4)]
            v = dft4(v)
            where = pl.ds(pl.multiple_of(g * 16, 16), 16)
            for m in range(4):
                row = j + 8 * m
                w = times(v[m], (lanes[0, row : row + 1], lanes[1, row : row + 1]))
                for p in range(2):
                    hi, lo = split(w[p])
                    z_hi[m, where, p * 128 : (p + 1) * 128] = hi
                    z_lo[m, where, p * 128 : (p + 1) * 128] = lo

        flat = p0.at[j].reshape(1024, 128)
        dims = (((1,), (1,)), ((), ()))
        for pair in range(2):
            hi = z_hi[pair * 2 : pair * 2 + 2].reshape(256, 256)
            lo = z_lo[pair * 2 : pair * 2 + 2].reshape(256, 256)
            both = lax.dot_general(h[...], hi, dims, preferred_element_type=F32)
            result = both[:256] + both[256:] + lax.dot_general(h[:256], lo, dims, preferred_element_type=F32)
            for p in range(2):
                for t in range(2):
                    flat[pl.ds(p * 4 + pair * 2 + t, 128, stride=8), :] = result[
                        p * 128 : p * 128 + 128, t * 128 : t * 128 + 128
                    ]

    buffers = (p0, p1, p2, p3)

    def leave(j, stage):
        src, dst, sem = buffers[stage].at[j], buffers[stage + 1].at[j], last_sem.at[stage, j]
        axis = ORDERS[j][stage]
        if axis == "z":
            for d in (2, 1, 3):
                to = (z + d) % 4
                send(src.at[to], dst.at[z], 4 + stage, sem, device(to, y, x, c))
            dst[z] = src[z]
        elif axis == "y":
            for d in (2, 1, 3):
                to = (y + d) % 4
                send(src.at[:, :, :, to], dst.at[:, :, :, y], 4 + stage, sem, device(z, to, x, c))
            dst[:, :, :, y] = src[:, :, :, y]
        else:
            for d, t in ((2, 1), (2, 0), (1, 1), (3, 1), (1, 0), (3, 0), (0, 1)):
                tx, tc = (x + d) % 4, (c + t) % 2
                send(src.at[:, tc, tx], dst.at[:, c, x], 4 + stage, sem, device(z, y, tx, tc))
            dst[:, c, x] = src[:, c, x]

    def arrive(j, stage):
        dst, sem = buffers[stage + 1].at[j], last_sem.at[stage, j]
        axis = ORDERS[j][stage]
        if axis == "z":
            landed(dst.at[pl.ds(0, 3)], sem)
        elif axis == "y":
            landed(dst.at[:, :, :, pl.ds(0, 3)], sem)
        else:
            flat = buffers[stage + 1].at[j].reshape(128, 8, 128)
            landed(flat.at[pl.ds(0, 112)], sem)

    def write(j):
        flat = p3.at[j].reshape(1024, 128)
        for p in range(2):
            for m in range(4):
                row = (j + 8 * m) * 128
                outputs[p][row : row + 128] = flat[pl.ds(p * 4 + m, 128, stride=8), :].T

    step_z(0)
    step_z(1)
    step_y(0)
    step_z(2)
    step_y(1)
    step_x(0)
    step_z(3)
    step_y(2)
    step_x(1)
    step_y(3)
    step_x(2)
    step_local(0)
    step_x(3)
    step_local(1)
    step_local(2)
    step_local(3)

    for j in range(8):
        finish(j)
        leave(j, 0)
    for j, stage in ((0, 0), (1, 0), (2, 0), (6, 0), (3, 0), (4, 0), (1, 1), (7, 0), (5, 0), (3, 1), (2, 1), (0, 1), (7, 1), (4, 1), (6, 1), (5, 1), (0, 2), (1, 2), (2, 2), (6, 2), (3, 2), (4, 2), (5, 2), (7, 2)):
        arrive(j, stage)
        if stage < 2:
            leave(j, stage + 1)
        else:
            write(j)

    def sent(ref, stage):
        pltpu.make_async_remote_copy(
            src_ref=ref, dst_ref=ref, send_sem=send_sem.at[stage], recv_sem=send_sem.at[stage],
            device_id=(me,), device_id_type=MESH,
        ).wait_send()

    sent(b1.at[pl.ds(0, 3)], 0)
    sent(b2.at[pl.ds(0, 3)], 1)
    sent(b3.at[:, :, pl.ds(0, 7)], 2)
    sent(b3.at[:, :, pl.ds(0, 7)], 3)
    for stage in range(3):
        eighths = sum(7 if order[stage] == "x" else 6 for order in ORDERS)
        sent(p0.reshape(64, 128, 128).at[pl.ds(0, eighths)], 4 + stage)


def store(re_ref, im_ref, out_re, out_im, sems):
    copies = [
        pltpu.make_async_copy(src.at[pl.ds(k * 512, 512)], dst.at[pl.ds(k * 512, 512)], sems.at[p, k])
        for k in range(8)
        for p, (src, dst) in enumerate(((re_ref, out_re), (im_ref, out_im)))
    ]
    for copy in copies:
        copy.start()
    for copy in copies:
        copy.wait()


def body(signal_real, signal_imag):
    shape = (4, 32, 32, 1, 128)
    block = (8, 4, 2, 4, 4, 8, 128)
    spectrum = pl.pallas_call(
        kernel,
        out_shape=[pltpu.VMEM((4096, 128), F32)] * 2,
        in_specs=[pl.BlockSpec(memory_space=pl.ANY)] * 2,
        out_specs=[pl.BlockSpec(memory_space=pltpu.VMEM)] * 2,
        scratch_shapes=[
            pltpu.VMEM((4, 2, 4, 8, 32, 128), F32),
            pltpu.VMEM((4, 2, 4, 8, 32, 128), F32),
            pltpu.VMEM((4, 2, 8, 8, 16, 128), F32),
            pltpu.VMEM((4, 2, 8, 8, 16, 128), F32),
            pltpu.VMEM(block, F32),
            pltpu.VMEM(block, F32),
            pltpu.VMEM(block, F32),
            pltpu.VMEM(block, F32),
            pltpu.VMEM((2, 32, 128, 128), F32),
            pltpu.VMEM((4, 128, 256), BF16),
            pltpu.VMEM((4, 128, 256), BF16),
            pltpu.VMEM((512, 256), BF16),
            pltpu.VMEM((512, 256), BF16),
            pltpu.VMEM((2, 32, 128), F32),
            pltpu.SemaphoreType.DMA((4,)),
            pltpu.SemaphoreType.DMA((7,)),
            pltpu.SemaphoreType.DMA((4, 4)),
            pltpu.SemaphoreType.DMA((3, 8)),
        ],
        compiler_params=pltpu.CompilerParams(collective_id=0, has_side_effects=True, vmem_limit_bytes=48 * 2**20),
    )(signal_real.reshape(shape), signal_imag.reshape(shape))
    out_re, out_im = pl.pallas_call(
        store,
        out_shape=[jax.ShapeDtypeStruct((4096, 128), F32)] * 2,
        in_specs=[pl.BlockSpec(memory_space=pltpu.VMEM)] * 2,
        out_specs=[pl.BlockSpec(memory_space=pl.ANY)] * 2,
        scratch_shapes=[pltpu.SemaphoreType.DMA((2, 8))],
        compiler_params=pltpu.CompilerParams(vmem_limit_bytes=8 * 2**20),
    )(*spectrum)
    return out_re.reshape(-1), out_im.reshape(-1)


def solution(mesh):
    return jax.shard_map(
        body, mesh=mesh, in_specs=(P("pa"), P("pa")), out_specs=(P("pa"), P("pa")), check_vma=False
    )
```

```python
import math

import jax
import jax.numpy as jnp
from jax import lax
from jax.experimental import pallas as pl
from jax.experimental.pallas import tpu as pltpu
from jax.sharding import PartitionSpec as P

MESH = pl.DeviceIdType.MESH
F32 = jnp.float32
BF16 = jnp.bfloat16
ROOT_HALF = math.sqrt(0.5)
ORDERS = ('yxz', 'zyx', 'xzy', 'zyx', 'xzy', 'xyz', 'yxz', 'zyx')


def device(z, y, x, c):
    return ((z * 4 + y) * 4 + x) * 2 + c


def unit_root(phase, bits):
    phase = phase & ((1 << bits) - 1)
    quarter = (phase + (1 << (bits - 3))) >> (bits - 2)
    angle = (phase - (quarter << (bits - 2))).astype(F32) * (2.0 * math.pi / (1 << bits))
    square = angle * angle
    sine = angle * (1.0 + square * (-1 / 6 + square * (1 / 120 + square * (-1 / 5040 + square * (1 / 362880)))))
    cosine = 1.0 + square * (-1 / 2 + square * (1 / 24 + square * (-1 / 720 + square * (1 / 40320))))
    odd = (quarter & 1) == 1
    real = jnp.where(odd, sine, cosine)
    imag = jnp.where(odd, cosine, sine)
    real = jnp.where(((quarter + 1) & 2) == 2, -real, real)
    imag = jnp.where((quarter & 2) == 2, imag, -imag)
    return real, imag


def times(value, factor):
    (a, b), (c, d) = value, factor
    return a * c - b * d, a * d + b * c


def plus(a, b):
    return a[0] + b[0], a[1] + b[1]


def minus(a, b):
    return a[0] - b[0], a[1] - b[1]


def dft4(v):
    s, d = plus(v[0], v[2]), minus(v[0], v[2])
    t, u = plus(v[1], v[3]), minus(v[1], v[3])
    return [plus(s, t), (d[0] + u[1], d[1] - u[0]), minus(s, t), (d[0] - u[1], d[1] + u[0])]


def dft8(v):
    even, odd = dft4(v[0::2]), dft4(v[1::2])
    turned = [
        odd[0],
        ((odd[1][0] + odd[1][1]) * ROOT_HALF, (odd[1][1] - odd[1][0]) * ROOT_HALF),
        (odd[2][1], -odd[2][0]),
        ((odd[3][1] - odd[3][0]) * ROOT_HALF, (odd[3][0] + odd[3][1]) * -ROOT_HALF),
    ]
    return [plus(e, t) for e, t in zip(even, turned)] + [minus(e, t) for e, t in zip(even, turned)]


def split(value):
    high = value.astype(BF16)
    return high, (value - high.astype(F32)).astype(BF16)


def kernel(
    re_hbm, im_hbm, out_re, out_im,
    b1, b2, b3, b4, p0, p1, p2, p3, turn, z_hi, z_lo, g, h, lanes, first,
    own_sem, first_sem, send_sem, recv_sem, last_sem,
):
    me = lax.axis_index("pa")
    z, y, x, c = me // 32, (me // 8) % 4, (me // 2) % 4, me % 2
    inputs, outputs = (re_hbm, im_hbm), (out_re, out_im)

    barrier = pltpu.get_barrier_semaphore()
    peers = [device((z + d) % 4, y, x, (c + t) % 2) for t in range(2) for d in (2, 1, 3)]
    peers += [device(z, y, (x + d) % 4, (c + t) % 2) for d in (2, 1, 3, 0) for t in range(2) if d + t]
    peers += [device(z, (y + d) % 4, x, c) for d in (2, 1, 3)]
    for peer in peers:
        pl.semaphore_signal(barrier, inc=1, device_id=(peer,), device_id_type=MESH)
    for part in range(2):

        @pl.loop(0, 8)
        def _(i):
            pltpu.make_async_copy(inputs[part].at[:, :, i * 4, 0], first.at[part, i], first_sem.at[part]).start()

    pl.semaphore_wait(barrier, len(peers))

    def send(src, dst, stage, sem, peer):
        pltpu.make_async_remote_copy(
            src_ref=src, dst_ref=dst, send_sem=send_sem.at[stage], recv_sem=sem, device_id=(peer,), device_id_type=MESH
        ).start()

    def landed(ref, sem):
        pltpu.make_async_remote_copy(
            src_ref=ref, dst_ref=ref, send_sem=sem, recv_sem=sem, device_id=(me,), device_id_type=MESH
        ).wait_recv()

    for part in range(2):
        pltpu.make_async_copy(first.at[part], first.at[part], first_sem.at[part]).wait()
        for d in (2, 1, 3):
            to = (z + d) % 4
            send(first.at[part, :, to], b1.at[0, part, z], 0, recv_sem.at[0, 0], device(to, y, x, c))
    for q in range(1, 4):
        for part in range(2):

            @pl.loop(0, 8)
            def _(i):
                for d in (2, 1, 3):
                    to = (z + d) % 4
                    send(
                        inputs[part].at[to, :, i * 4 + q, 0],
                        b1.at[q, part, z, i],
                        0, recv_sem.at[0, q], device(to, y, x, c),
                    )
                pltpu.make_async_copy(
                    inputs[part].at[z, :, i * 4 + q, 0], b1.at[q, part, z, i], own_sem.at[q]
                ).start()
    for part in range(2):
        b1[0, part, z] = first[part, :, z]

    s = z * 32 + c * 16 + x * 4 + y
    rows = lax.broadcasted_iota(jnp.int32, (128, 128), 0)
    cols = lax.broadcasted_iota(jnp.int32, (128, 128), 1)

    def matrix(phase, bits, scale, table):
        real, imag = unit_root(phase, bits)
        real, imag = real * scale, imag * scale
        for r, k, block in ((0, 0, real), (0, 1, -imag), (1, 0, imag), (1, 1, real)):
            hi, lo = split(block)
            table[r * 128 : r * 128 + 128, k * 128 : k * 128 + 128] = hi
            table[r * 128 + 256 : r * 128 + 384, k * 128 : k * 128 + 128] = lo

    matrix((rows * 128 + s) * cols, 14, 1.0, g)
    target = (rows & 96) + (rows & 3) * 8 + ((rows >> 2) & 3) * 2 + ((rows >> 4) & 1)
    matrix(target * cols, 7, 1.0 / 8192.0, h)
    lane_rows = lax.broadcasted_iota(jnp.int32, (32, 128), 0)
    lane_cols = lax.broadcasted_iota(jnp.int32, (32, 128), 1)
    lanes[0], lanes[1] = unit_root(lane_rows * lane_cols, 12)

    @pl.loop(0, 32)
    def _(f):
        real, imag = unit_root((rows * 128 + s) * (cols + f * 128), 26)
        turn[0, f] = real
        turn[1, f] = imag

    def scalar_root(phase, bits):
        return unit_root(jnp.full((8, 128), 1, jnp.int32) * phase, bits)

    turn_y = [scalar_root(k * y, 4) for k in range(4)]
    turn_x = [scalar_root((4 * k + y) * (2 * x + c), 7) for k in range(4)]

    def four(buf, q, factors):
        @pl.loop(0, 8)
        def _(i):
            v = [tuple(buf[q, p, k, i].reshape(4, 8, 128) for p in range(2)) for k in range(4)]
            v = [times(o, (w[0][None], w[1][None])) for o, w in zip(dft4(v), factors)]
            for k in range(4):
                for p in range(2):
                    buf[q, p, k, i] = v[k][p].reshape(32, 128)

    def step_z(q):
        landed(b1.at[q, :, pl.ds(0, 3)], recv_sem.at[0, q])
        if q:
            pltpu.make_async_copy(b1.at[q, :, 0], b1.at[q, :, 0], own_sem.at[q]).wait()
        four(b1, q, turn_y)
        for d in (2, 1, 3):
            to = (y + d) % 4
            send(b1.at[q, :, to], b2.at[q, :, y], 1, recv_sem.at[1, q], device(z, to, x, c))
        for p in range(2):
            b2[q, p, y] = b1[q, p, y]

    def step_y(q):
        landed(b2.at[q, :, pl.ds(0, 3)], recv_sem.at[1, q])
        four(b2, q, turn_x)
        for d, t in ((2, 1), (2, 0), (1, 1), (3, 1), (1, 0), (3, 0), (0, 1)):
            tx, tc = (x + d) % 4, (c + t) % 2
            send(
                b2.at[q, :, tx, :, pl.ds(pl.multiple_of(tc * 16, 16), 16)],
                b3.at[q, :, x * 2 + c],
                2, recv_sem.at[2, q], device(z, y, tx, tc),
            )
        for p in range(2):
            b3[q, p, x * 2 + c] = b2[q, p, x, :, pl.ds(pl.multiple_of(c * 16, 16), 16)]

    def step_x(q):
        landed(b3.at[q, :, pl.ds(0, 7)], recv_sem.at[2, q])

        @pl.loop(0, 8)
        def _(i):
            v = dft8([(b3[q, 0, k, i], b3[q, 1, k, i]) for k in range(8)])
            for k in range(8):
                b3[q, 0, k, i] = v[k][0]
                b3[q, 1, k, i] = v[k][1]

        def leave_x(tz, tc):
            send(
                b3.at[q, :, tz * 2 + tc],
                b4.at[q, :, :, z * 2 + c],
                3, recv_sem.at[3, q], device(tz, y, x, tc),
            )

        leave_x(z, 1 - c)
        for tc in range(2):
            for d in (2, 1, 3):
                leave_x((z + d) % 4, tc)
        for p in range(2):
            b4[q, p, :, z * 2 + c] = b3[q, p, z * 2 + c]

    def step_local(q):
        landed(b4.at[q, :, :, pl.ds(0, 7)], recv_sem.at[3, q])

        @pl.loop(0, 4, unroll=True)
        def _(pair):
            block = jnp.concatenate(
                [
                    jnp.concatenate([b4[q, p, pair * 2 + t].reshape(128, 128) for t in range(2)], axis=1)
                    for p in range(2)
                ],
                axis=0,
            )
            hi, lo = split(block)
            both = jnp.dot(g[...], hi, preferred_element_type=F32)
            result = both[:256] + both[256:] + jnp.dot(g[:256], lo, preferred_element_type=F32)
            for t in range(2):
                f = (pair * 2 + t) * 4 + q
                value = (result[:128, t * 128 : t * 128 + 128], result[128:, t * 128 : t * 128 + 128])
                value = times(value, (turn[0, f], turn[1, f]))
                for p in range(2):
                    b4[q, p, pair * 2 + t] = value[p].reshape(8, 16, 128)

        @pl.loop(0, 8, unroll=True)
        def _(g):
            v = dft8([(b4[q, 0, i, g], b4[q, 1, i, g]) for i in range(8)])
            for i in range(8):
                b4[q, 0, i, g] = v[i][0]
                b4[q, 1, i, g] = v[i][1]

    def finish(j):
        roots = [
            (math.cos(-2 * math.pi * q * j / 32), math.sin(-2 * math.pi * q * j / 32)) for q in range(4)
        ]

        @pl.loop(0, 8, unroll=True)
        def _(g):
            v = [(b4[q, 0, j, g], b4[q, 1, j, g]) for q in range(4)]
            if j:
                v = [v[0]] + [times(v[q], roots[q]) for q in range(1, 4)]
            v = dft4(v)
            where = pl.ds(pl.multiple_of(g * 16, 16), 16)
            for m in range(4):
                row = j + 8 * m
                w = times(v[m], (lanes[0, row : row + 1], lanes[1, row : row + 1]))
                for p in range(2):
                    hi, lo = split(w[p])
                    z_hi[m, where, p * 128 : (p + 1) * 128] = hi
                    z_lo[m, where, p * 128 : (p + 1) * 128] = lo

        flat = p0.at[j].reshape(1024, 128)
        dims = (((1,), (1,)), ((), ()))
        for pair in range(2):
            hi = z_hi[pair * 2 : pair * 2 + 2].reshape(256, 256)
            lo = z_lo[pair * 2 : pair * 2 + 2].reshape(256, 256)
            both = lax.dot_general(h[...], hi, dims, preferred_element_type=F32)
            result = both[:256] + both[256:] + lax.dot_general(h[:256], lo, dims, preferred_element_type=F32)
            for p in range(2):
                for t in range(2):
                    flat[pl.ds(p * 4 + pair * 2 + t, 128, stride=8), :] = result[
                        p * 128 : p * 128 + 128, t * 128 : t * 128 + 128
                    ]

    buffers = (p0, p1, p2, p3)

    def leave(j, stage):
        src, dst, sem = buffers[stage].at[j], buffers[stage + 1].at[j], last_sem.at[stage, j]
        axis = ORDERS[j][stage]
        if axis == "z":
            for d in (2, 1, 3):
                to = (z + d) % 4
                send(src.at[to], dst.at[z], 4 + stage, sem, device(to, y, x, c))
            dst[z] = src[z]
        elif axis == "y":
            for d in (2, 1, 3):
                to = (y + d) % 4
                send(src.at[:, :, :, to], dst.at[:, :, :, y], 4 + stage, sem, device(z, to, x, c))
            dst[:, :, :, y] = src[:, :, :, y]
        else:
            for d, t in ((2, 1), (2, 0), (1, 1), (3, 1), (1, 0), (3, 0), (0, 1)):
                tx, tc = (x + d) % 4, (c + t) % 2
                send(src.at[:, tc, tx], dst.at[:, c, x], 4 + stage, sem, device(z, y, tx, tc))
            dst[:, c, x] = src[:, c, x]

    def arrive(j, stage):
        dst, sem = buffers[stage + 1].at[j], last_sem.at[stage, j]
        axis = ORDERS[j][stage]
        if axis == "z":
            landed(dst.at[pl.ds(0, 3)], sem)
        elif axis == "y":
            landed(dst.at[:, :, :, pl.ds(0, 3)], sem)
        else:
            flat = buffers[stage + 1].at[j].reshape(128, 8, 128)
            landed(flat.at[pl.ds(0, 112)], sem)

    def write(j):
        flat = p3.at[j].reshape(1024, 128)
        for p in range(2):
            for m in range(4):
                row = (j + 8 * m) * 128
                outputs[p][row : row + 128] = flat[pl.ds(p * 4 + m, 128, stride=8), :].T

    step_z(0)
    step_z(1)
    step_y(0)
    step_z(2)
    step_y(1)
    step_x(0)
    step_z(3)
    step_y(2)
    step_x(1)
    step_y(3)
    step_x(2)
    step_local(0)
    step_x(3)
    step_local(1)
    step_local(2)
    step_local(3)

    for j in range(8):
        finish(j)
        leave(j, 0)
    for j, stage in ((0, 0), (1, 0), (2, 0), (6, 0), (3, 0), (4, 0), (1, 1), (7, 0), (5, 0), (3, 1), (2, 1), (0, 1), (7, 1), (4, 1), (6, 1), (5, 1), (0, 2), (1, 2), (2, 2), (6, 2), (3, 2), (4, 2), (5, 2), (7, 2)):
        arrive(j, stage)
        if stage < 2:
            leave(j, stage + 1)
        else:
            write(j)

    def sent(ref, stage):
        pltpu.make_async_remote_copy(
            src_ref=ref, dst_ref=ref, send_sem=send_sem.at[stage], recv_sem=send_sem.at[stage],
            device_id=(me,), device_id_type=MESH,
        ).wait_send()

    sent(b1.at[pl.ds(0, 3)], 0)
    sent(b2.at[pl.ds(0, 3)], 1)
    sent(b3.at[:, :, pl.ds(0, 7)], 2)
    sent(b3.at[:, :, pl.ds(0, 7)], 3)
    for stage in range(3):
        eighths = sum(7 if order[stage] == "x" else 6 for order in ORDERS)
        sent(p0.reshape(64, 128, 128).at[pl.ds(0, eighths)], 4 + stage)


def store(re_ref, im_ref, out_re, out_im, sems):
    copies = [
        pltpu.make_async_copy(src.at[pl.ds(k * 512, 512)], dst.at[pl.ds(k * 512, 512)], sems.at[p, k])
        for k in range(8)
        for p, (src, dst) in enumerate(((re_ref, out_re), (im_ref, out_im)))
    ]
    for copy in copies:
        copy.start()
    for copy in copies:
        copy.wait()


def body(signal_real, signal_imag):
    shape = (4, 32, 32, 1, 128)
    block = (8, 4, 2, 4, 4, 8, 128)
    spectrum = pl.pallas_call(
        kernel,
        out_shape=[pltpu.VMEM((4096, 128), F32)] * 2,
        in_specs=[pl.BlockSpec(memory_space=pl.ANY)] * 2,
        out_specs=[pl.BlockSpec(memory_space=pltpu.VMEM)] * 2,
        scratch_shapes=[
            pltpu.VMEM((4, 2, 4, 8, 32, 128), F32),
            pltpu.VMEM((4, 2, 4, 8, 32, 128), F32),
            pltpu.VMEM((4, 2, 8, 8, 16, 128), F32),
            pltpu.VMEM((4, 2, 8, 8, 16, 128), F32),
            pltpu.VMEM(block, F32),
            pltpu.VMEM(block, F32),
            pltpu.VMEM(block, F32),
            pltpu.VMEM(block, F32),
            pltpu.VMEM((2, 32, 128, 128), F32),
            pltpu.VMEM((4, 128, 256), BF16),
            pltpu.VMEM((4, 128, 256), BF16),
            pltpu.VMEM((512, 256), BF16),
            pltpu.VMEM((512, 256), BF16),
            pltpu.VMEM((2, 32, 128), F32),
            pltpu.VMEM((2, 8, 4, 32, 128), F32),
            pltpu.SemaphoreType.DMA((4,)),
            pltpu.SemaphoreType.DMA((2,)),
            pltpu.SemaphoreType.DMA((7,)),
            pltpu.SemaphoreType.DMA((4, 4)),
            pltpu.SemaphoreType.DMA((3, 8)),
        ],
        compiler_params=pltpu.CompilerParams(collective_id=0, has_side_effects=True, vmem_limit_bytes=48 * 2**20),
    )(signal_real.reshape(shape), signal_imag.reshape(shape))
    out_re, out_im = pl.pallas_call(
        store,
        out_shape=[jax.ShapeDtypeStruct((4096, 128), F32)] * 2,
        in_specs=[pl.BlockSpec(memory_space=pltpu.VMEM)] * 2,
        out_specs=[pl.BlockSpec(memory_space=pl.ANY)] * 2,
        scratch_shapes=[pltpu.SemaphoreType.DMA((2, 8))],
        compiler_params=pltpu.CompilerParams(vmem_limit_bytes=8 * 2**20),
    )(*spectrum)
    return out_re.reshape(-1), out_im.reshape(-1)


def solution(mesh):
    return jax.shard_map(
        body, mesh=mesh, in_specs=(P("pa"), P("pa")), out_specs=(P("pa"), P("pa")), check_vma=False
    )
```

```python
import math

import jax
import jax.numpy as jnp
from jax import lax
from jax.experimental import pallas as pl
from jax.experimental.pallas import tpu as pltpu
from jax.sharding import PartitionSpec as P

MESH = pl.DeviceIdType.MESH
F32 = jnp.float32
BF16 = jnp.bfloat16
ROOT_HALF = math.sqrt(0.5)
ORDERS = ('yxz', 'zyx', 'xzy', 'zyx', 'xzy', 'xyz', 'yxz', 'zyx')


def device(z, y, x, c):
    return ((z * 4 + y) * 4 + x) * 2 + c


def unit_root(phase, bits):
    phase = phase & ((1 << bits) - 1)
    quarter = (phase + (1 << (bits - 3))) >> (bits - 2)
    angle = (phase - (quarter << (bits - 2))).astype(F32) * (2.0 * math.pi / (1 << bits))
    square = angle * angle
    sine = angle * (1.0 + square * (-1 / 6 + square * (1 / 120 + square * (-1 / 5040 + square * (1 / 362880)))))
    cosine = 1.0 + square * (-1 / 2 + square * (1 / 24 + square * (-1 / 720 + square * (1 / 40320))))
    odd = (quarter & 1) == 1
    real = jnp.where(odd, sine, cosine)
    imag = jnp.where(odd, cosine, sine)
    real = jnp.where(((quarter + 1) & 2) == 2, -real, real)
    imag = jnp.where((quarter & 2) == 2, imag, -imag)
    return real, imag


def times(value, factor):
    (a, b), (c, d) = value, factor
    return a * c - b * d, a * d + b * c


def plus(a, b):
    return a[0] + b[0], a[1] + b[1]


def minus(a, b):
    return a[0] - b[0], a[1] - b[1]


def dft4(v):
    s, d = plus(v[0], v[2]), minus(v[0], v[2])
    t, u = plus(v[1], v[3]), minus(v[1], v[3])
    return [plus(s, t), (d[0] + u[1], d[1] - u[0]), minus(s, t), (d[0] - u[1], d[1] + u[0])]


def dft8(v):
    even, odd = dft4(v[0::2]), dft4(v[1::2])
    turned = [
        odd[0],
        ((odd[1][0] + odd[1][1]) * ROOT_HALF, (odd[1][1] - odd[1][0]) * ROOT_HALF),
        (odd[2][1], -odd[2][0]),
        ((odd[3][1] - odd[3][0]) * ROOT_HALF, (odd[3][0] + odd[3][1]) * -ROOT_HALF),
    ]
    return [plus(e, t) for e, t in zip(even, turned)] + [minus(e, t) for e, t in zip(even, turned)]


def split(value):
    high = value.astype(BF16)
    return high, (value - high.astype(F32)).astype(BF16)


def kernel(
    re_hbm, im_hbm, out_re, out_im,
    b1, b2, b3, b4, p0, p1, p2, p3, turn, z_hi, z_lo, g, h, lanes, first,
    own_sem, first_sem, send_sem, recv_sem, last_sem,
):
    me = lax.axis_index("pa")
    z, y, x, c = me // 32, (me // 8) % 4, (me // 2) % 4, me % 2
    inputs, outputs = (re_hbm, im_hbm), (out_re, out_im)

    barrier = pltpu.get_barrier_semaphore()
    peers = [device((z + d) % 4, y, x, (c + t) % 2) for t in range(2) for d in (2, 1, 3)]
    peers += [device(z, y, (x + d) % 4, (c + t) % 2) for d in (2, 1, 3, 0) for t in range(2) if d + t]
    peers += [device(z, (y + d) % 4, x, c) for d in (2, 1, 3)]
    for peer in peers:
        pl.semaphore_signal(barrier, inc=1, device_id=(peer,), device_id_type=MESH)
    for part in range(2):

        @pl.loop(0, 8)
        def _(i):
            pltpu.make_async_copy(inputs[part].at[:, :, i * 4, 0], first.at[part, i], first_sem.at[part]).start()

    pl.semaphore_wait(barrier, len(peers))

    def send(src, dst, stage, sem, peer):
        pltpu.make_async_remote_copy(
            src_ref=src, dst_ref=dst, send_sem=send_sem.at[stage], recv_sem=sem, device_id=(peer,), device_id_type=MESH
        ).start()

    def landed(ref, sem):
        pltpu.make_async_remote_copy(
            src_ref=ref, dst_ref=ref, send_sem=sem, recv_sem=sem, device_id=(me,), device_id_type=MESH
        ).wait_recv()

    for part in range(2):
        pltpu.make_async_copy(first.at[part], first.at[part], first_sem.at[part]).wait()
        for d in (2, 1, 3):
            to = (z + d) % 4
            send(first.at[part, :, to], b1.at[0, part, z], 0, recv_sem.at[0, 0], device(to, y, x, c))
    for q in range(1, 4):
        for part in range(2):

            @pl.loop(0, 8)
            def _(i):
                for d in (2, 1, 3):
                    to = (z + d) % 4
                    send(
                        inputs[part].at[to, :, i * 4 + q, 0],
                        b1.at[q, part, z, i],
                        0, recv_sem.at[0, q], device(to, y, x, c),
                    )
                pltpu.make_async_copy(
                    inputs[part].at[z, :, i * 4 + q, 0], b1.at[q, part, z, i], own_sem.at[q]
                ).start()
    for part in range(2):
        b1[0, part, z] = first[part, :, z]

    s = z * 32 + c * 16 + x * 4 + y
    rows = lax.broadcasted_iota(jnp.int32, (128, 128), 0)
    cols = lax.broadcasted_iota(jnp.int32, (128, 128), 1)

    def matrix(phase, bits, scale, table):
        real, imag = unit_root(phase, bits)
        real, imag = real * scale, imag * scale
        for r, k, block in ((0, 0, real), (0, 1, -imag), (1, 0, imag), (1, 1, real)):
            hi, lo = split(block)
            table[r * 128 : r * 128 + 128, k * 128 : k * 128 + 128] = hi
            table[r * 128 + 256 : r * 128 + 384, k * 128 : k * 128 + 128] = lo

    matrix((rows * 128 + s) * cols, 14, 1.0, g)
    target = (rows & 96) + (rows & 3) * 8 + ((rows >> 2) & 3) * 2 + ((rows >> 4) & 1)
    matrix(target * cols, 7, 1.0 / 8192.0, h)
    lane_rows = lax.broadcasted_iota(jnp.int32, (32, 128), 0)
    lane_cols = lax.broadcasted_iota(jnp.int32, (32, 128), 1)
    lanes[0], lanes[1] = unit_root(lane_rows * lane_cols, 12)

    @pl.loop(0, 32)
    def _(f):
        real, imag = unit_root((rows * 128 + s) * (cols + f * 128), 26)
        turn[0, f] = real
        turn[1, f] = imag

    def scalar_root(phase, bits):
        return unit_root(jnp.full((8, 128), 1, jnp.int32) * phase, bits)

    turn_y = [scalar_root(k * y, 4) for k in range(4)]
    turn_x = [scalar_root((4 * k + y) * (2 * x + c), 7) for k in range(4)]

    def four(buf, q, factors):
        @pl.loop(0, 8)
        def _(i):
            v = [tuple(buf[q, p, k, i].reshape(4, 8, 128) for p in range(2)) for k in range(4)]
            v = [times(o, (w[0][None], w[1][None])) for o, w in zip(dft4(v), factors)]
            for k in range(4):
                for p in range(2):
                    buf[q, p, k, i] = v[k][p].reshape(32, 128)

    def step_z(q):
        landed(b1.at[q, :, pl.ds(0, 3)], recv_sem.at[0, q])
        if q:
            pltpu.make_async_copy(b1.at[q, :, 0], b1.at[q, :, 0], own_sem.at[q]).wait()
        four(b1, q, turn_y)
        for d in (2, 1, 3):
            to = (y + d) % 4
            send(b1.at[q, :, to], b2.at[q, :, y], 1, recv_sem.at[1, q], device(z, to, x, c))
        for p in range(2):
            b2[q, p, y] = b1[q, p, y]

    def step_y(q):
        landed(b2.at[q, :, pl.ds(0, 3)], recv_sem.at[1, q])
        four(b2, q, turn_x)
        for d, t in ((2, 1), (2, 0), (1, 1), (3, 1), (1, 0), (3, 0), (0, 1)):
            tx, tc = (x + d) % 4, (c + t) % 2
            send(
                b2.at[q, :, tx, :, pl.ds(pl.multiple_of(tc * 16, 16), 16)],
                b3.at[q, :, x * 2 + c],
                2, recv_sem.at[2, q], device(z, y, tx, tc),
            )
        for p in range(2):
            b3[q, p, x * 2 + c] = b2[q, p, x, :, pl.ds(pl.multiple_of(c * 16, 16), 16)]

    def step_x(q):
        landed(b3.at[q, :, pl.ds(0, 7)], recv_sem.at[2, q])

        @pl.loop(0, 8)
        def _(i):
            v = dft8([(b3[q, 0, k, i], b3[q, 1, k, i]) for k in range(8)])
            for k in range(8):
                b3[q, 0, k, i] = v[k][0]
                b3[q, 1, k, i] = v[k][1]

        def leave_x(tz, tc):
            send(
                b3.at[q, :, tz * 2 + tc],
                b4.at[q, :, :, z * 2 + c],
                3, recv_sem.at[3, q], device(tz, y, x, tc),
            )

        leave_x(z, 1 - c)
        for tc in (1, 0):
            for d in (2, 1, 3):
                leave_x((z + d) % 4, tc)
        for p in range(2):
            b4[q, p, :, z * 2 + c] = b3[q, p, z * 2 + c]

    def step_local(q):
        landed(b4.at[q, :, :, pl.ds(0, 7)], recv_sem.at[3, q])

        @pl.loop(0, 4, unroll=True)
        def _(pair):
            block = jnp.concatenate(
                [
                    jnp.concatenate([b4[q, p, pair * 2 + t].reshape(128, 128) for t in range(2)], axis=1)
                    for p in range(2)
                ],
                axis=0,
            )
            hi, lo = split(block)
            both = jnp.dot(g[...], hi, preferred_element_type=F32)
            result = both[:256] + both[256:] + jnp.dot(g[:256], lo, preferred_element_type=F32)
            for t in range(2):
                f = (pair * 2 + t) * 4 + q
                value = (result[:128, t * 128 : t * 128 + 128], result[128:, t * 128 : t * 128 + 128])
                value = times(value, (turn[0, f], turn[1, f]))
                for p in range(2):
                    b4[q, p, pair * 2 + t] = value[p].reshape(8, 16, 128)

        @pl.loop(0, 8, unroll=True)
        def _(g):
            v = dft8([(b4[q, 0, i, g], b4[q, 1, i, g]) for i in range(8)])
            for i in range(8):
                b4[q, 0, i, g] = v[i][0]
                b4[q, 1, i, g] = v[i][1]

    def finish(j):
        roots = [
            (math.cos(-2 * math.pi * q * j / 32), math.sin(-2 * math.pi * q * j / 32)) for q in range(4)
        ]

        @pl.loop(0, 8, unroll=True)
        def _(g):
            v = [(b4[q, 0, j, g], b4[q, 1, j, g]) for q in range(4)]
            if j:
                v = [v[0]] + [times(v[q], roots[q]) for q in range(1, 4)]
            v = dft4(v)
            where = pl.ds(pl.multiple_of(g * 16, 16), 16)
            for m in range(4):
                row = j + 8 * m
                w = times(v[m], (lanes[0, row : row + 1], lanes[1, row : row + 1]))
                for p in range(2):
                    hi, lo = split(w[p])
                    z_hi[m, where, p * 128 : (p + 1) * 128] = hi
                    z_lo[m, where, p * 128 : (p + 1) * 128] = lo

        flat = p0.at[j].reshape(1024, 128)
        dims = (((1,), (1,)), ((), ()))
        for pair in range(2):
            hi = z_hi[pair * 2 : pair * 2 + 2].reshape(256, 256)
            lo = z_lo[pair * 2 : pair * 2 + 2].reshape(256, 256)
            both = lax.dot_general(h[...], hi, dims, preferred_element_type=F32)
            result = both[:256] + both[256:] + lax.dot_general(h[:256], lo, dims, preferred_element_type=F32)
            for p in range(2):
                for t in range(2):
                    flat[pl.ds(p * 4 + pair * 2 + t, 128, stride=8), :] = result[
                        p * 128 : p * 128 + 128, t * 128 : t * 128 + 128
                    ]

    buffers = (p0, p1, p2, p3)

    def leave(j, stage):
        src, dst, sem = buffers[stage].at[j], buffers[stage + 1].at[j], last_sem.at[stage, j]
        axis = ORDERS[j][stage]
        if axis == "z":
            for d in (2, 1, 3):
                to = (z + d) % 4
                send(src.at[to], dst.at[z], 4 + stage, sem, device(to, y, x, c))
            dst[z] = src[z]
        elif axis == "y":
            for d in (2, 1, 3):
                to = (y + d) % 4
                send(src.at[:, :, :, to], dst.at[:, :, :, y], 4 + stage, sem, device(z, to, x, c))
            dst[:, :, :, y] = src[:, :, :, y]
        else:
            for d, t in ((2, 1), (2, 0), (1, 1), (3, 1), (1, 0), (3, 0), (0, 1)):
                tx, tc = (x + d) % 4, (c + t) % 2
                send(src.at[:, tc, tx], dst.at[:, c, x], 4 + stage, sem, device(z, y, tx, tc))
            dst[:, c, x] = src[:, c, x]

    def arrive(j, stage):
        dst, sem = buffers[stage + 1].at[j], last_sem.at[stage, j]
        axis = ORDERS[j][stage]
        if axis == "z":
            landed(dst.at[pl.ds(0, 3)], sem)
        elif axis == "y":
            landed(dst.at[:, :, :, pl.ds(0, 3)], sem)
        else:
            flat = buffers[stage + 1].at[j].reshape(128, 8, 128)
            landed(flat.at[pl.ds(0, 112)], sem)

    def write(j):
        flat = p3.at[j].reshape(1024, 128)
        for p in range(2):
            for m in range(4):
                row = (j + 8 * m) * 128
                outputs[p][row : row + 128] = flat[pl.ds(p * 4 + m, 128, stride=8), :].T

    step_z(0)
    step_z(1)
    step_y(0)
    step_z(2)
    step_y(1)
    step_x(0)
    step_z(3)
    step_y(2)
    step_x(1)
    step_y(3)
    step_x(2)
    step_local(0)
    step_x(3)
    step_local(1)
    step_local(2)
    step_local(3)

    for j in range(8):
        finish(j)
        leave(j, 0)
    for j, stage in ((0, 0), (1, 0), (2, 0), (6, 0), (3, 0), (4, 0), (1, 1), (7, 0), (5, 0), (3, 1), (2, 1), (0, 1), (7, 1), (4, 1), (6, 1), (5, 1), (0, 2), (1, 2), (2, 2), (6, 2), (3, 2), (4, 2), (5, 2), (7, 2)):
        arrive(j, stage)
        if stage < 2:
            leave(j, stage + 1)
        else:
            write(j)

    def sent(ref, stage):
        pltpu.make_async_remote_copy(
            src_ref=ref, dst_ref=ref, send_sem=send_sem.at[stage], recv_sem=send_sem.at[stage],
            device_id=(me,), device_id_type=MESH,
        ).wait_send()

    sent(b1.at[pl.ds(0, 3)], 0)
    sent(b2.at[pl.ds(0, 3)], 1)
    sent(b3.at[:, :, pl.ds(0, 7)], 2)
    sent(b3.at[:, :, pl.ds(0, 7)], 3)
    for stage in range(3):
        eighths = sum(7 if order[stage] == "x" else 6 for order in ORDERS)
        sent(p0.reshape(64, 128, 128).at[pl.ds(0, eighths)], 4 + stage)


def store(re_ref, im_ref, out_re, out_im, sems):
    copies = [
        pltpu.make_async_copy(src.at[pl.ds(k * 512, 512)], dst.at[pl.ds(k * 512, 512)], sems.at[p, k])
        for k in range(8)
        for p, (src, dst) in enumerate(((re_ref, out_re), (im_ref, out_im)))
    ]
    for copy in copies:
        copy.start()
    for copy in copies:
        copy.wait()


def body(signal_real, signal_imag):
    shape = (4, 32, 32, 1, 128)
    block = (8, 4, 2, 4, 4, 8, 128)
    spectrum = pl.pallas_call(
        kernel,
        out_shape=[pltpu.VMEM((4096, 128), F32)] * 2,
        in_specs=[pl.BlockSpec(memory_space=pl.ANY)] * 2,
        out_specs=[pl.BlockSpec(memory_space=pltpu.VMEM)] * 2,
        scratch_shapes=[
            pltpu.VMEM((4, 2, 4, 8, 32, 128), F32),
            pltpu.VMEM((4, 2, 4, 8, 32, 128), F32),
            pltpu.VMEM((4, 2, 8, 8, 16, 128), F32),
            pltpu.VMEM((4, 2, 8, 8, 16, 128), F32),
            pltpu.VMEM(block, F32),
            pltpu.VMEM(block, F32),
            pltpu.VMEM(block, F32),
            pltpu.VMEM(block, F32),
            pltpu.VMEM((2, 32, 128, 128), F32),
            pltpu.VMEM((4, 128, 256), BF16),
            pltpu.VMEM((4, 128, 256), BF16),
            pltpu.VMEM((512, 256), BF16),
            pltpu.VMEM((512, 256), BF16),
            pltpu.VMEM((2, 32, 128), F32),
            pltpu.VMEM((2, 8, 4, 32, 128), F32),
            pltpu.SemaphoreType.DMA((4,)),
            pltpu.SemaphoreType.DMA((2,)),
            pltpu.SemaphoreType.DMA((7,)),
            pltpu.SemaphoreType.DMA((4, 4)),
            pltpu.SemaphoreType.DMA((3, 8)),
        ],
        compiler_params=pltpu.CompilerParams(collective_id=0, has_side_effects=True, vmem_limit_bytes=48 * 2**20),
    )(signal_real.reshape(shape), signal_imag.reshape(shape))
    out_re, out_im = pl.pallas_call(
        store,
        out_shape=[jax.ShapeDtypeStruct((4096, 128), F32)] * 2,
        in_specs=[pl.BlockSpec(memory_space=pltpu.VMEM)] * 2,
        out_specs=[pl.BlockSpec(memory_space=pl.ANY)] * 2,
        scratch_shapes=[pltpu.SemaphoreType.DMA((2, 8))],
        compiler_params=pltpu.CompilerParams(vmem_limit_bytes=8 * 2**20),
    )(*spectrum)
    return out_re.reshape(-1), out_im.reshape(-1)


def solution(mesh):
    return jax.shard_map(
        body, mesh=mesh, in_specs=(P("pa"), P("pa")), out_specs=(P("pa"), P("pa")), check_vma=False
    )
```

```python
import math

import jax
import jax.numpy as jnp
from jax import lax
from jax.experimental import pallas as pl
from jax.experimental.pallas import tpu as pltpu
from jax.sharding import PartitionSpec as P

MESH = pl.DeviceIdType.MESH
F32 = jnp.float32
BF16 = jnp.bfloat16
ROOT_HALF = math.sqrt(0.5)
ORDERS = ('yxz', 'zyx', 'xzy', 'zyx', 'xzy', 'xyz', 'yxz', 'zyx')


def device(z, y, x, c):
    return ((z * 4 + y) * 4 + x) * 2 + c


def unit_root(phase, bits):
    phase = phase & ((1 << bits) - 1)
    quarter = (phase + (1 << (bits - 3))) >> (bits - 2)
    angle = (phase - (quarter << (bits - 2))).astype(F32) * (2.0 * math.pi / (1 << bits))
    square = angle * angle
    sine = angle * (1.0 + square * (-1 / 6 + square * (1 / 120 + square * (-1 / 5040 + square * (1 / 362880)))))
    cosine = 1.0 + square * (-1 / 2 + square * (1 / 24 + square * (-1 / 720 + square * (1 / 40320))))
    odd = (quarter & 1) == 1
    real = jnp.where(odd, sine, cosine)
    imag = jnp.where(odd, cosine, sine)
    real = jnp.where(((quarter + 1) & 2) == 2, -real, real)
    imag = jnp.where((quarter & 2) == 2, imag, -imag)
    return real, imag


def times(value, factor):
    (a, b), (c, d) = value, factor
    return a * c - b * d, a * d + b * c


def plus(a, b):
    return a[0] + b[0], a[1] + b[1]


def minus(a, b):
    return a[0] - b[0], a[1] - b[1]


def dft4(v):
    s, d = plus(v[0], v[2]), minus(v[0], v[2])
    t, u = plus(v[1], v[3]), minus(v[1], v[3])
    return [plus(s, t), (d[0] + u[1], d[1] - u[0]), minus(s, t), (d[0] - u[1], d[1] + u[0])]


def dft8(v):
    even, odd = dft4(v[0::2]), dft4(v[1::2])
    turned = [
        odd[0],
        ((odd[1][0] + odd[1][1]) * ROOT_HALF, (odd[1][1] - odd[1][0]) * ROOT_HALF),
        (odd[2][1], -odd[2][0]),
        ((odd[3][1] - odd[3][0]) * ROOT_HALF, (odd[3][0] + odd[3][1]) * -ROOT_HALF),
    ]
    return [plus(e, t) for e, t in zip(even, turned)] + [minus(e, t) for e, t in zip(even, turned)]


def split(value):
    high = value.astype(BF16)
    return high, (value - high.astype(F32)).astype(BF16)


def kernel(
    re_hbm, im_hbm, out_re, out_im,
    b1, b2, b3, b4, p0, p1, p2, p3, turn, z_hi, z_lo, g, h, lanes, first,
    own_sem, first_sem, send_sem, recv_sem, last_sem,
):
    me = lax.axis_index("pa")
    z, y, x, c = me // 32, (me // 8) % 4, (me // 2) % 4, me % 2
    inputs, outputs = (re_hbm, im_hbm), (out_re, out_im)

    barrier = pltpu.get_barrier_semaphore()
    peers = [device((z + d) % 4, y, x, (c + t) % 2) for t in range(2) for d in (2, 1, 3)]
    peers += [device(z, y, (x + d) % 4, (c + t) % 2) for d in (2, 1, 3, 0) for t in range(2) if d + t]
    peers += [device(z, (y + d) % 4, x, c) for d in (2, 1, 3)]
    for peer in peers:
        pl.semaphore_signal(barrier, inc=1, device_id=(peer,), device_id_type=MESH)
    for part in range(2):

        @pl.loop(0, 8)
        def _(i):
            pltpu.make_async_copy(inputs[part].at[:, :, i * 4, 0], first.at[part, i], first_sem.at[part]).start()

    pl.semaphore_wait(barrier, len(peers))

    def send(src, dst, stage, sem, peer):
        pltpu.make_async_remote_copy(
            src_ref=src, dst_ref=dst, send_sem=send_sem.at[stage], recv_sem=sem, device_id=(peer,), device_id_type=MESH
        ).start()

    def landed(ref, sem):
        pltpu.make_async_remote_copy(
            src_ref=ref, dst_ref=ref, send_sem=sem, recv_sem=sem, device_id=(me,), device_id_type=MESH
        ).wait_recv()

    for part in range(2):
        pltpu.make_async_copy(first.at[part], first.at[part], first_sem.at[part]).wait()
        for d in (2, 1, 3):
            to = (z + d) % 4
            send(first.at[part, :, to], b1.at[0, part, z], 0, recv_sem.at[0, 0], device(to, y, x, c))
    for q in range(1, 4):
        for part in range(2):

            @pl.loop(0, 8)
            def _(i):
                for d in (2, 1, 3):
                    to = (z + d) % 4
                    send(
                        inputs[part].at[to, :, i * 4 + q, 0],
                        b1.at[q, part, z, i],
                        0, recv_sem.at[0, q], device(to, y, x, c),
                    )
                pltpu.make_async_copy(
                    inputs[part].at[z, :, i * 4 + q, 0], b1.at[q, part, z, i], own_sem.at[q]
                ).start()
    for part in range(2):
        b1[0, part, z] = first[part, :, z]

    s = z * 32 + c * 16 + x * 4 + y
    rows = lax.broadcasted_iota(jnp.int32, (128, 128), 0)
    cols = lax.broadcasted_iota(jnp.int32, (128, 128), 1)

    def matrix(phase, bits, scale, table):
        real, imag = unit_root(phase, bits)
        real, imag = real * scale, imag * scale
        for r, k, block in ((0, 0, real), (0, 1, -imag), (1, 0, imag), (1, 1, real)):
            hi, lo = split(block)
            table[r * 128 : r * 128 + 128, k * 128 : k * 128 + 128] = hi
            table[r * 128 + 256 : r * 128 + 384, k * 128 : k * 128 + 128] = lo

    matrix((rows * 128 + s) * cols, 14, 1.0, g)
    target = (rows & 96) + (rows & 3) * 8 + ((rows >> 2) & 3) * 2 + ((rows >> 4) & 1)
    matrix(target * cols, 7, 1.0 / 8192.0, h)
    lane_rows = lax.broadcasted_iota(jnp.int32, (32, 128), 0)
    lane_cols = lax.broadcasted_iota(jnp.int32, (32, 128), 1)
    lanes[0], lanes[1] = unit_root(lane_rows * lane_cols, 12)

    @pl.loop(0, 32)
    def _(f):
        real, imag = unit_root((rows * 128 + s) * (cols + f * 128), 26)
        turn[0, f] = real
        turn[1, f] = imag

    def scalar_root(phase, bits):
        return unit_root(jnp.full((8, 128), 1, jnp.int32) * phase, bits)

    turn_y = [scalar_root(k * y, 4) for k in range(4)]
    turn_x = [scalar_root((4 * k + y) * (2 * x + c), 7) for k in range(4)]

    def four(buf, q, factors):
        @pl.loop(0, 8)
        def _(i):
            v = [tuple(buf[q, p, k, i].reshape(4, 8, 128) for p in range(2)) for k in range(4)]
            v = [times(o, (w[0][None], w[1][None])) for o, w in zip(dft4(v), factors)]
            for k in range(4):
                for p in range(2):
                    buf[q, p, k, i] = v[k][p].reshape(32, 128)

    def step_z(q):
        landed(b1.at[q, :, pl.ds(0, 3)], recv_sem.at[0, q])
        if q:
            pltpu.make_async_copy(b1.at[q, :, 0], b1.at[q, :, 0], own_sem.at[q]).wait()
        four(b1, q, turn_y)
        for d in (2, 1, 3):
            to = (y + d) % 4
            send(b1.at[q, :, to], b2.at[q, :, y], 1, recv_sem.at[1, q], device(z, to, x, c))
        for p in range(2):
            b2[q, p, y] = b1[q, p, y]

    def step_y(q):
        landed(b2.at[q, :, pl.ds(0, 3)], recv_sem.at[1, q])
        four(b2, q, turn_x)
        for d, t in ((2, 1), (2, 0), (1, 1), (3, 1), (1, 0), (3, 0), (0, 1)):
            tx, tc = (x + d) % 4, (c + t) % 2
            send(
                b2.at[q, :, tx, :, pl.ds(pl.multiple_of(tc * 16, 16), 16)],
                b3.at[q, :, x * 2 + c],
                2, recv_sem.at[2, q], device(z, y, tx, tc),
            )
        for p in range(2):
            b3[q, p, x * 2 + c] = b2[q, p, x, :, pl.ds(pl.multiple_of(c * 16, 16), 16)]

    def step_x(q):
        landed(b3.at[q, :, pl.ds(0, 7)], recv_sem.at[2, q])

        @pl.loop(0, 8)
        def _(i):
            v = dft8([(b3[q, 0, k, i], b3[q, 1, k, i]) for k in range(8)])
            for k in range(8):
                b3[q, 0, k, i] = v[k][0]
                b3[q, 1, k, i] = v[k][1]

        def leave_x(tz, tc):
            send(
                b3.at[q, :, tz * 2 + tc],
                b4.at[q, :, :, z * 2 + c],
                3, recv_sem.at[3, q], device(tz, y, x, tc),
            )

        leave_x(z, 1 - c)
        for tc in (1, 0):
            for d in (2, 1, 3):
                leave_x((z + d) % 4, tc)
        for p in range(2):
            b4[q, p, :, z * 2 + c] = b3[q, p, z * 2 + c]

    def step_local(q):
        landed(b4.at[q, :, :, pl.ds(0, 7)], recv_sem.at[3, q])

        @pl.loop(0, 4, unroll=True)
        def _(pair):
            block = jnp.concatenate(
                [
                    jnp.concatenate([b4[q, p, pair * 2 + t].reshape(128, 128) for t in range(2)], axis=1)
                    for p in range(2)
                ],
                axis=0,
            )
            hi, lo = split(block)
            both = jnp.dot(g[...], hi, preferred_element_type=F32)
            result = both[:256] + both[256:] + jnp.dot(g[:256], lo, preferred_element_type=F32)
            for t in range(2):
                f = (pair * 2 + t) * 4 + q
                value = (result[:128, t * 128 : t * 128 + 128], result[128:, t * 128 : t * 128 + 128])
                value = times(value, (turn[0, f], turn[1, f]))
                for p in range(2):
                    b4[q, p, pair * 2 + t] = value[p].reshape(8, 16, 128)

        @pl.loop(0, 8, unroll=True)
        def _(g):
            v = dft8([(b4[q, 0, i, g], b4[q, 1, i, g]) for i in range(8)])
            for i in range(8):
                b4[q, 0, i, g] = v[i][0]
                b4[q, 1, i, g] = v[i][1]

    def finish(j):
        roots = [
            (math.cos(-2 * math.pi * q * j / 32), math.sin(-2 * math.pi * q * j / 32)) for q in range(4)
        ]

        @pl.loop(0, 8, unroll=True)
        def _(g):
            v = [(b4[q, 0, j, g], b4[q, 1, j, g]) for q in range(4)]
            if j:
                v = [v[0]] + [times(v[q], roots[q]) for q in range(1, 4)]
            v = dft4(v)
            where = pl.ds(pl.multiple_of(g * 16, 16), 16)
            for m in range(4):
                row = j + 8 * m
                w = times(v[m], (lanes[0, row : row + 1], lanes[1, row : row + 1]))
                for p in range(2):
                    hi, lo = split(w[p])
                    z_hi[m, where, p * 128 : (p + 1) * 128] = hi
                    z_lo[m, where, p * 128 : (p + 1) * 128] = lo

        flat = p0.at[j].reshape(1024, 128)
        dims = (((1,), (1,)), ((), ()))
        for pair in range(2):
            hi = z_hi[pair * 2 : pair * 2 + 2].reshape(256, 256)
            lo = z_lo[pair * 2 : pair * 2 + 2].reshape(256, 256)
            both = lax.dot_general(h[...], hi, dims, preferred_element_type=F32)
            result = both[:256] + both[256:] + lax.dot_general(h[:256], lo, dims, preferred_element_type=F32)
            for p in range(2):
                for t in range(2):
                    flat[pl.ds(p * 4 + pair * 2 + t, 128, stride=8), :] = result[
                        p * 128 : p * 128 + 128, t * 128 : t * 128 + 128
                    ]

    buffers = (p0, p1, p2, p3)

    def leave(j, stage):
        src, dst, sem = buffers[stage].at[j], buffers[stage + 1].at[j], last_sem.at[stage, j]
        axis = ORDERS[j][stage]
        if axis == "z":
            for d in (2, 1, 3):
                to = (z + d) % 4
                send(src.at[to], dst.at[z], 4 + stage, sem, device(to, y, x, c))
            dst[z] = src[z]
        elif axis == "y":
            for d in (2, 1, 3):
                to = (y + d) % 4
                send(src.at[:, :, :, to], dst.at[:, :, :, y], 4 + stage, sem, device(z, to, x, c))
            dst[:, :, :, y] = src[:, :, :, y]
        else:
            send(src.at[:, 1 - c, x], dst.at[:, c, x], 4 + stage, sem, device(z, y, x, 1 - c))
            for tc in (1, 0):
                for d in (2, 1, 3):
                    tx = (x + d) % 4
                    send(src.at[:, tc, tx], dst.at[:, c, x], 4 + stage, sem, device(z, y, tx, tc))
            dst[:, c, x] = src[:, c, x]

    def arrive(j, stage):
        dst, sem = buffers[stage + 1].at[j], last_sem.at[stage, j]
        axis = ORDERS[j][stage]
        if axis == "z":
            landed(dst.at[pl.ds(0, 3)], sem)
        elif axis == "y":
            landed(dst.at[:, :, :, pl.ds(0, 3)], sem)
        else:
            flat = buffers[stage + 1].at[j].reshape(128, 8, 128)
            landed(flat.at[pl.ds(0, 112)], sem)

    def write(j):
        flat = p3.at[j].reshape(1024, 128)
        for p in range(2):
            for m in range(4):
                row = (j + 8 * m) * 128
                outputs[p][row : row + 128] = flat[pl.ds(p * 4 + m, 128, stride=8), :].T

    step_z(0)
    step_z(1)
    step_y(0)
    step_z(2)
    step_y(1)
    step_x(0)
    step_z(3)
    step_y(2)
    step_x(1)
    step_y(3)
    step_x(2)
    step_local(0)
    step_x(3)
    step_local(1)
    step_local(2)
    step_local(3)

    for j in range(8):
        finish(j)
        leave(j, 0)
    for j, stage in ((0, 0), (1, 0), (2, 0), (6, 0), (3, 0), (4, 0), (1, 1), (7, 0), (5, 0), (3, 1), (2, 1), (0, 1), (7, 1), (4, 1), (6, 1), (5, 1), (0, 2), (1, 2), (2, 2), (6, 2), (3, 2), (4, 2), (5, 2), (7, 2)):
        arrive(j, stage)
        if stage < 2:
            leave(j, stage + 1)
        else:
            write(j)

    def sent(ref, stage):
        pltpu.make_async_remote_copy(
            src_ref=ref, dst_ref=ref, send_sem=send_sem.at[stage], recv_sem=send_sem.at[stage],
            device_id=(me,), device_id_type=MESH,
        ).wait_send()

    sent(b1.at[pl.ds(0, 3)], 0)
    sent(b2.at[pl.ds(0, 3)], 1)
    sent(b3.at[:, :, pl.ds(0, 7)], 2)
    sent(b3.at[:, :, pl.ds(0, 7)], 3)
    for stage in range(3):
        eighths = sum(7 if order[stage] == "x" else 6 for order in ORDERS)
        sent(p0.reshape(64, 128, 128).at[pl.ds(0, eighths)], 4 + stage)


def store(re_ref, im_ref, out_re, out_im, sems):
    copies = [
        pltpu.make_async_copy(src.at[pl.ds(k * 512, 512)], dst.at[pl.ds(k * 512, 512)], sems.at[p, k])
        for k in range(8)
        for p, (src, dst) in enumerate(((re_ref, out_re), (im_ref, out_im)))
    ]
    for copy in copies:
        copy.start()
    for copy in copies:
        copy.wait()


def body(signal_real, signal_imag):
    shape = (4, 32, 32, 1, 128)
    block = (8, 4, 2, 4, 4, 8, 128)
    spectrum = pl.pallas_call(
        kernel,
        out_shape=[pltpu.VMEM((4096, 128), F32)] * 2,
        in_specs=[pl.BlockSpec(memory_space=pl.ANY)] * 2,
        out_specs=[pl.BlockSpec(memory_space=pltpu.VMEM)] * 2,
        scratch_shapes=[
            pltpu.VMEM((4, 2, 4, 8, 32, 128), F32),
            pltpu.VMEM((4, 2, 4, 8, 32, 128), F32),
            pltpu.VMEM((4, 2, 8, 8, 16, 128), F32),
            pltpu.VMEM((4, 2, 8, 8, 16, 128), F32),
            pltpu.VMEM(block, F32),
            pltpu.VMEM(block, F32),
            pltpu.VMEM(block, F32),
            pltpu.VMEM(block, F32),
            pltpu.VMEM((2, 32, 128, 128), F32),
            pltpu.VMEM((4, 128, 256), BF16),
            pltpu.VMEM((4, 128, 256), BF16),
            pltpu.VMEM((512, 256), BF16),
            pltpu.VMEM((512, 256), BF16),
            pltpu.VMEM((2, 32, 128), F32),
            pltpu.VMEM((2, 8, 4, 32, 128), F32),
            pltpu.SemaphoreType.DMA((4,)),
            pltpu.SemaphoreType.DMA((2,)),
            pltpu.SemaphoreType.DMA((7,)),
            pltpu.SemaphoreType.DMA((4, 4)),
            pltpu.SemaphoreType.DMA((3, 8)),
        ],
        compiler_params=pltpu.CompilerParams(collective_id=0, has_side_effects=True, vmem_limit_bytes=48 * 2**20),
    )(signal_real.reshape(shape), signal_imag.reshape(shape))
    out_re, out_im = pl.pallas_call(
        store,
        out_shape=[jax.ShapeDtypeStruct((4096, 128), F32)] * 2,
        in_specs=[pl.BlockSpec(memory_space=pltpu.VMEM)] * 2,
        out_specs=[pl.BlockSpec(memory_space=pl.ANY)] * 2,
        scratch_shapes=[pltpu.SemaphoreType.DMA((2, 8))],
        compiler_params=pltpu.CompilerParams(vmem_limit_bytes=8 * 2**20),
    )(*spectrum)
    return out_re.reshape(-1), out_im.reshape(-1)


def solution(mesh):
    return jax.shard_map(
        body, mesh=mesh, in_specs=(P("pa"), P("pa")), out_specs=(P("pa"), P("pa")), check_vma=False
    )
```

```python
import math

import jax
import jax.numpy as jnp
from jax import lax
from jax.experimental import pallas as pl
from jax.experimental.pallas import tpu as pltpu
from jax.sharding import PartitionSpec as P

MESH = pl.DeviceIdType.MESH
F32 = jnp.float32
BF16 = jnp.bfloat16
ROOT_HALF = math.sqrt(0.5)
ORDERS = ('yxz', 'zyx', 'xzy', 'zyx', 'xzy', 'xyz', 'yxz', 'zyx')


def device(z, y, x, c):
    return ((z * 4 + y) * 4 + x) * 2 + c


def unit_root(phase, bits):
    phase = phase & ((1 << bits) - 1)
    quarter = (phase + (1 << (bits - 3))) >> (bits - 2)
    angle = (phase - (quarter << (bits - 2))).astype(F32) * (2.0 * math.pi / (1 << bits))
    square = angle * angle
    sine = angle * (1.0 + square * (-1 / 6 + square * (1 / 120 + square * (-1 / 5040 + square * (1 / 362880)))))
    cosine = 1.0 + square * (-1 / 2 + square * (1 / 24 + square * (-1 / 720 + square * (1 / 40320))))
    odd = (quarter & 1) == 1
    real = jnp.where(odd, sine, cosine)
    imag = jnp.where(odd, cosine, sine)
    real = jnp.where(((quarter + 1) & 2) == 2, -real, real)
    imag = jnp.where((quarter & 2) == 2, imag, -imag)
    return real, imag


def times(value, factor):
    (a, b), (c, d) = value, factor
    return a * c - b * d, a * d + b * c


def plus(a, b):
    return a[0] + b[0], a[1] + b[1]


def minus(a, b):
    return a[0] - b[0], a[1] - b[1]


def dft4(v):
    s, d = plus(v[0], v[2]), minus(v[0], v[2])
    t, u = plus(v[1], v[3]), minus(v[1], v[3])
    return [plus(s, t), (d[0] + u[1], d[1] - u[0]), minus(s, t), (d[0] - u[1], d[1] + u[0])]


def dft8(v):
    even, odd = dft4(v[0::2]), dft4(v[1::2])
    turned = [
        odd[0],
        ((odd[1][0] + odd[1][1]) * ROOT_HALF, (odd[1][1] - odd[1][0]) * ROOT_HALF),
        (odd[2][1], -odd[2][0]),
        ((odd[3][1] - odd[3][0]) * ROOT_HALF, (odd[3][0] + odd[3][1]) * -ROOT_HALF),
    ]
    return [plus(e, t) for e, t in zip(even, turned)] + [minus(e, t) for e, t in zip(even, turned)]


def split(value):
    high = value.astype(BF16)
    return high, (value - high.astype(F32)).astype(BF16)


def kernel(
    re_hbm, im_hbm, out_re, out_im,
    b1, b2, b3, b4, p0, p1, p2, p3, turn, z_hi, z_lo, g, h, lanes, first,
    own_sem, first_sem, send_sem, recv_sem, last_sem,
):
    me = lax.axis_index("pa")
    z, y, x, c = me // 32, (me // 8) % 4, (me // 2) % 4, me % 2
    inputs, outputs = (re_hbm, im_hbm), (out_re, out_im)

    barrier = pltpu.get_barrier_semaphore()
    peers = [device((z + d) % 4, y, x, (c + t) % 2) for t in range(2) for d in (2, 1, 3)]
    peers += [device(z, y, (x + d) % 4, (c + t) % 2) for d in (2, 1, 3, 0) for t in range(2) if d + t]
    peers += [device(z, (y + d) % 4, x, c) for d in (2, 1, 3)]
    for peer in peers:
        pl.semaphore_signal(barrier, inc=1, device_id=(peer,), device_id_type=MESH)
    for part in range(2):

        @pl.loop(0, 8)
        def _(i):
            pltpu.make_async_copy(inputs[part].at[:, :, i * 4, 0], first.at[part, i], first_sem.at[part]).start()

    pl.semaphore_wait(barrier, len(peers))

    def send(src, dst, stage, sem, peer):
        pltpu.make_async_remote_copy(
            src_ref=src, dst_ref=dst, send_sem=send_sem.at[stage], recv_sem=sem, device_id=(peer,), device_id_type=MESH
        ).start()

    def landed(ref, sem):
        pltpu.make_async_remote_copy(
            src_ref=ref, dst_ref=ref, send_sem=sem, recv_sem=sem, device_id=(me,), device_id_type=MESH
        ).wait_recv()

    for part in range(2):
        pltpu.make_async_copy(first.at[part], first.at[part], first_sem.at[part]).wait()
        for d in (2, 1, 3):
            to = (z + d) % 4
            send(first.at[part, :, to], b1.at[0, part, z], 0, recv_sem.at[0, 0], device(to, y, x, c))
    for q in range(1, 4):
        for part in range(2):

            @pl.loop(0, 8)
            def _(i):
                for d in (2, 1, 3):
                    to = (z + d) % 4
                    send(
                        inputs[part].at[to, :, i * 4 + q, 0],
                        b1.at[q, part, z, i],
                        0, recv_sem.at[0, q], device(to, y, x, c),
                    )
                pltpu.make_async_copy(
                    inputs[part].at[z, :, i * 4 + q, 0], b1.at[q, part, z, i], own_sem.at[q]
                ).start()
    for part in range(2):
        b1[0, part, z] = first[part, :, z]

    s = z * 32 + c * 16 + x * 4 + y
    rows = lax.broadcasted_iota(jnp.int32, (128, 128), 0)
    cols = lax.broadcasted_iota(jnp.int32, (128, 128), 1)

    def matrix(phase, bits, scale, table):
        real, imag = unit_root(phase, bits)
        real, imag = real * scale, imag * scale
        for r, k, block in ((0, 0, real), (0, 1, -imag), (1, 0, imag), (1, 1, real)):
            hi, lo = split(block)
            table[r * 128 : r * 128 + 128, k * 128 : k * 128 + 128] = hi
            table[r * 128 + 256 : r * 128 + 384, k * 128 : k * 128 + 128] = lo

    matrix((rows * 128 + s) * cols, 14, 1.0, g)
    target = (rows & 96) + (rows & 3) * 8 + ((rows >> 2) & 3) * 2 + ((rows >> 4) & 1)
    matrix(target * cols, 7, 1.0 / 8192.0, h)
    lane_rows = lax.broadcasted_iota(jnp.int32, (32, 128), 0)
    lane_cols = lax.broadcasted_iota(jnp.int32, (32, 128), 1)
    lanes[0], lanes[1] = unit_root(lane_rows * lane_cols, 12)

    @pl.loop(0, 32)
    def _(f):
        real, imag = unit_root((rows * 128 + s) * (cols + f * 128), 26)
        turn[0, f] = real
        turn[1, f] = imag

    def scalar_root(phase, bits):
        return unit_root(jnp.full((8, 128), 1, jnp.int32) * phase, bits)

    turn_y = [scalar_root(k * y, 4) for k in range(4)]
    turn_x = [scalar_root((4 * k + y) * (2 * x + c), 7) for k in range(4)]

    def four(buf, q, factors):
        @pl.loop(0, 8)
        def _(i):
            v = [tuple(buf[q, p, k, i].reshape(4, 8, 128) for p in range(2)) for k in range(4)]
            v = [times(o, (w[0][None], w[1][None])) for o, w in zip(dft4(v), factors)]
            for k in range(4):
                for p in range(2):
                    buf[q, p, k, i] = v[k][p].reshape(32, 128)

    def step_z(q):
        landed(b1.at[q, :, pl.ds(0, 3)], recv_sem.at[0, q])
        if q:
            pltpu.make_async_copy(b1.at[q, :, 0], b1.at[q, :, 0], own_sem.at[q]).wait()
        four(b1, q, turn_y)
        for d in (2, 1, 3):
            to = (y + d) % 4
            send(b1.at[q, :, to], b2.at[q, :, y], 1, recv_sem.at[1, q], device(z, to, x, c))
        for p in range(2):
            b2[q, p, y] = b1[q, p, y]

    def step_y(q):
        landed(b2.at[q, :, pl.ds(0, 3)], recv_sem.at[1, q])
        four(b2, q, turn_x)
        for d, t in ((2, 1), (2, 0), (1, 1), (3, 1), (1, 0), (3, 0), (0, 1)):
            tx, tc = (x + d) % 4, (c + t) % 2
            send(
                b2.at[q, :, tx, :, pl.ds(pl.multiple_of(tc * 16, 16), 16)],
                b3.at[q, :, x * 2 + c],
                2, recv_sem.at[2, q], device(z, y, tx, tc),
            )
        for p in range(2):
            b3[q, p, x * 2 + c] = b2[q, p, x, :, pl.ds(pl.multiple_of(c * 16, 16), 16)]

    def step_x(q):
        landed(b3.at[q, :, pl.ds(0, 7)], recv_sem.at[2, q])

        @pl.loop(0, 8)
        def _(i):
            v = dft8([(b3[q, 0, k, i], b3[q, 1, k, i]) for k in range(8)])
            for k in range(8):
                b3[q, 0, k, i] = v[k][0]
                b3[q, 1, k, i] = v[k][1]

        def leave_x(tz, tc):
            send(
                b3.at[q, :, tz * 2 + tc],
                b4.at[q, :, :, z * 2 + c],
                3, recv_sem.at[3, q], device(tz, y, x, tc),
            )

        leave_x(z, 1 - c)
        for tc in (1, 0):
            for d in (2, 1, 3):
                leave_x((z + d) % 4, tc)
        for p in range(2):
            b4[q, p, :, z * 2 + c] = b3[q, p, z * 2 + c]

    def step_local(q):
        landed(b4.at[q, :, :, pl.ds(0, 7)], recv_sem.at[3, q])

        @pl.loop(0, 4, unroll=True)
        def _(pair):
            block = jnp.concatenate(
                [
                    jnp.concatenate([b4[q, p, pair * 2 + t].reshape(128, 128) for t in range(2)], axis=1)
                    for p in range(2)
                ],
                axis=0,
            )
            hi, lo = split(block)
            both = jnp.dot(g[...], hi, preferred_element_type=F32)
            result = both[:256] + both[256:] + jnp.dot(g[:256], lo, preferred_element_type=F32)
            for t in range(2):
                f = (pair * 2 + t) * 4 + q
                value = (result[:128, t * 128 : t * 128 + 128], result[128:, t * 128 : t * 128 + 128])
                value = times(value, (turn[0, f], turn[1, f]))
                for p in range(2):
                    b4[q, p, pair * 2 + t] = value[p].reshape(8, 16, 128)

        @pl.loop(0, 8, unroll=True)
        def _(g):
            v = dft8([(b4[q, 0, i, g], b4[q, 1, i, g]) for i in range(8)])
            for i in range(8):
                b4[q, 0, i, g] = v[i][0]
                b4[q, 1, i, g] = v[i][1]

    def finish(j):
        roots = [
            (math.cos(-2 * math.pi * q * j / 32), math.sin(-2 * math.pi * q * j / 32)) for q in range(4)
        ]

        @pl.loop(0, 8, unroll=True)
        def _(g):
            v = [(b4[q, 0, j, g], b4[q, 1, j, g]) for q in range(4)]
            if j:
                v = [v[0]] + [times(v[q], roots[q]) for q in range(1, 4)]
            v = dft4(v)
            where = pl.ds(pl.multiple_of(g * 16, 16), 16)
            for m in range(4):
                row = j + 8 * m
                w = times(v[m], (lanes[0, row : row + 1], lanes[1, row : row + 1]))
                for p in range(2):
                    hi, lo = split(w[p])
                    z_hi[m, where, p * 128 : (p + 1) * 128] = hi
                    z_lo[m, where, p * 128 : (p + 1) * 128] = lo

        flat = p0.at[j].reshape(1024, 128)
        dims = (((1,), (1,)), ((), ()))
        for pair in range(2):
            hi = z_hi[pair * 2 : pair * 2 + 2].reshape(256, 256)
            lo = z_lo[pair * 2 : pair * 2 + 2].reshape(256, 256)
            both = lax.dot_general(h[...], hi, dims, preferred_element_type=F32)
            result = both[:256] + both[256:] + lax.dot_general(h[:256], lo, dims, preferred_element_type=F32)
            for p in range(2):
                for t in range(2):
                    flat[pl.ds(p * 4 + pair * 2 + t, 128, stride=8), :] = result[
                        p * 128 : p * 128 + 128, t * 128 : t * 128 + 128
                    ]

    buffers = (p0, p1, p2, p3)

    def leave(j, stage):
        src, dst, sem = buffers[stage].at[j], buffers[stage + 1].at[j], last_sem.at[stage, j]
        axis = ORDERS[j][stage]
        if axis == "z":
            for d in (2, 1, 3):
                to = (z + d) % 4
                send(src.at[to], dst.at[z], 4 + stage, sem, device(to, y, x, c))
            dst[z] = src[z]
        elif axis == "y":
            for d in (2, 1, 3):
                to = (y + d) % 4
                send(src.at[:, :, :, to], dst.at[:, :, :, y], 4 + stage, sem, device(z, to, x, c))
            dst[:, :, :, y] = src[:, :, :, y]
        else:
            for d, t in ((2, 1), (2, 0), (1, 1), (3, 1), (1, 0), (3, 0), (0, 1)):
                tx, tc = (x + d) % 4, (c + t) % 2
                send(src.at[:, tc, tx], dst.at[:, c, x], 4 + stage, sem, device(z, y, tx, tc))
            dst[:, c, x] = src[:, c, x]

    def arrive(j, stage):
        dst, sem = buffers[stage + 1].at[j], last_sem.at[stage, j]
        axis = ORDERS[j][stage]
        if axis == "z":
            landed(dst.at[pl.ds(0, 3)], sem)
        elif axis == "y":
            landed(dst.at[:, :, :, pl.ds(0, 3)], sem)
        else:
            flat = buffers[stage + 1].at[j].reshape(128, 8, 128)
            landed(flat.at[pl.ds(0, 112)], sem)

    def write(j):
        flat = p3.at[j].reshape(1024, 128)
        for p in range(2):
            for m in range(4):
                row = (j + 8 * m) * 128
                outputs[p][row : row + 128] = flat[pl.ds(p * 4 + m, 128, stride=8), :].T

    step_z(0)
    step_z(1)
    step_y(0)
    step_z(2)
    step_y(1)
    step_x(0)
    step_z(3)
    step_y(2)
    step_x(1)
    step_y(3)
    step_x(2)
    step_local(0)
    step_x(3)
    step_local(1)
    step_local(2)
    step_local(3)

    for j in range(8):
        finish(j)
        leave(j, 0)
    def sent(ref, stage):
        pltpu.make_async_remote_copy(
            src_ref=ref, dst_ref=ref, send_sem=send_sem.at[stage], recv_sem=send_sem.at[stage],
            device_id=(me,), device_id_type=MESH,
        ).wait_send()

    def sent_last(stage):
        eighths = sum(7 if order[stage] == "x" else 6 for order in ORDERS)
        sent(p0.reshape(64, 128, 128).at[pl.ds(0, eighths)], 4 + stage)

    for j, stage in ((0, 0), (1, 0), (2, 0), (6, 0), (3, 0), (4, 0), (1, 1), (7, 0), (5, 0), (3, 1), (2, 1), (0, 1), (7, 1), (4, 1), (6, 1), (5, 1), (0, 2), (1, 2), (2, 2), (6, 2), (3, 2), (4, 2), (5, 2), (7, 2)):
        if (j, stage) == (5, 2):
            sent(b1.at[pl.ds(0, 3)], 0)
            sent(b2.at[pl.ds(0, 3)], 1)
            sent(b3.at[:, :, pl.ds(0, 7)], 2)
            sent(b3.at[:, :, pl.ds(0, 7)], 3)
            sent_last(0)
            sent_last(1)
        arrive(j, stage)
        if stage < 2:
            leave(j, stage + 1)
        else:
            write(j)
    sent_last(2)


def store(re_ref, im_ref, out_re, out_im, sems):
    copies = [
        pltpu.make_async_copy(src.at[pl.ds(k * 512, 512)], dst.at[pl.ds(k * 512, 512)], sems.at[p, k])
        for k in range(8)
        for p, (src, dst) in enumerate(((re_ref, out_re), (im_ref, out_im)))
    ]
    for copy in copies:
        copy.start()
    for copy in copies:
        copy.wait()


def body(signal_real, signal_imag):
    shape = (4, 32, 32, 1, 128)
    block = (8, 4, 2, 4, 4, 8, 128)
    spectrum = pl.pallas_call(
        kernel,
        out_shape=[pltpu.VMEM((4096, 128), F32)] * 2,
        in_specs=[pl.BlockSpec(memory_space=pl.ANY)] * 2,
        out_specs=[pl.BlockSpec(memory_space=pltpu.VMEM)] * 2,
        scratch_shapes=[
            pltpu.VMEM((4, 2, 4, 8, 32, 128), F32),
            pltpu.VMEM((4, 2, 4, 8, 32, 128), F32),
            pltpu.VMEM((4, 2, 8, 8, 16, 128), F32),
            pltpu.VMEM((4, 2, 8, 8, 16, 128), F32),
            pltpu.VMEM(block, F32),
            pltpu.VMEM(block, F32),
            pltpu.VMEM(block, F32),
            pltpu.VMEM(block, F32),
            pltpu.VMEM((2, 32, 128, 128), F32),
            pltpu.VMEM((4, 128, 256), BF16),
            pltpu.VMEM((4, 128, 256), BF16),
            pltpu.VMEM((512, 256), BF16),
            pltpu.VMEM((512, 256), BF16),
            pltpu.VMEM((2, 32, 128), F32),
            pltpu.VMEM((2, 8, 4, 32, 128), F32),
            pltpu.SemaphoreType.DMA((4,)),
            pltpu.SemaphoreType.DMA((2,)),
            pltpu.SemaphoreType.DMA((7,)),
            pltpu.SemaphoreType.DMA((4, 4)),
            pltpu.SemaphoreType.DMA((3, 8)),
        ],
        compiler_params=pltpu.CompilerParams(collective_id=0, has_side_effects=True, vmem_limit_bytes=48 * 2**20),
    )(signal_real.reshape(shape), signal_imag.reshape(shape))
    out_re, out_im = pl.pallas_call(
        store,
        out_shape=[jax.ShapeDtypeStruct((4096, 128), F32)] * 2,
        in_specs=[pl.BlockSpec(memory_space=pltpu.VMEM)] * 2,
        out_specs=[pl.BlockSpec(memory_space=pl.ANY)] * 2,
        scratch_shapes=[pltpu.SemaphoreType.DMA((2, 8))],
        compiler_params=pltpu.CompilerParams(vmem_limit_bytes=8 * 2**20),
    )(*spectrum)
    return out_re.reshape(-1), out_im.reshape(-1)


def solution(mesh):
    return jax.shard_map(
        body, mesh=mesh, in_specs=(P("pa"), P("pa")), out_specs=(P("pa"), P("pa")), check_vma=False
    )
```

```python
import math

import jax
import jax.numpy as jnp
from jax import lax
from jax.experimental import pallas as pl
from jax.experimental.pallas import tpu as pltpu
from jax.sharding import PartitionSpec as P

MESH = pl.DeviceIdType.MESH
F32 = jnp.float32
BF16 = jnp.bfloat16
ROOT_HALF = math.sqrt(0.5)
ORDERS = ('yxz', 'zyx', 'xzy', 'zyx', 'xzy', 'xyz', 'yxz', 'zyx')


def device(z, y, x, c):
    return ((z * 4 + y) * 4 + x) * 2 + c


def unit_root(phase, bits):
    phase = phase & ((1 << bits) - 1)
    quarter = (phase + (1 << (bits - 3))) >> (bits - 2)
    angle = (phase - (quarter << (bits - 2))).astype(F32) * (2.0 * math.pi / (1 << bits))
    square = angle * angle
    sine = angle * (1.0 + square * (-1 / 6 + square * (1 / 120 + square * (-1 / 5040 + square * (1 / 362880)))))
    cosine = 1.0 + square * (-1 / 2 + square * (1 / 24 + square * (-1 / 720 + square * (1 / 40320))))
    odd = (quarter & 1) == 1
    real = jnp.where(odd, sine, cosine)
    imag = jnp.where(odd, cosine, sine)
    real = jnp.where(((quarter + 1) & 2) == 2, -real, real)
    imag = jnp.where((quarter & 2) == 2, imag, -imag)
    return real, imag


def times(value, factor):
    (a, b), (c, d) = value, factor
    return a * c - b * d, a * d + b * c


def plus(a, b):
    return a[0] + b[0], a[1] + b[1]


def minus(a, b):
    return a[0] - b[0], a[1] - b[1]


def dft4(v):
    s, d = plus(v[0], v[2]), minus(v[0], v[2])
    t, u = plus(v[1], v[3]), minus(v[1], v[3])
    return [plus(s, t), (d[0] + u[1], d[1] - u[0]), minus(s, t), (d[0] - u[1], d[1] + u[0])]


def dft8(v):
    even, odd = dft4(v[0::2]), dft4(v[1::2])
    turned = [
        odd[0],
        ((odd[1][0] + odd[1][1]) * ROOT_HALF, (odd[1][1] - odd[1][0]) * ROOT_HALF),
        (odd[2][1], -odd[2][0]),
        ((odd[3][1] - odd[3][0]) * ROOT_HALF, (odd[3][0] + odd[3][1]) * -ROOT_HALF),
    ]
    return [plus(e, t) for e, t in zip(even, turned)] + [minus(e, t) for e, t in zip(even, turned)]


def split(value):
    high = value.astype(BF16)
    return high, (value - high.astype(F32)).astype(BF16)


def kernel(
    re_hbm, im_hbm, out_re, out_im,
    b1, b2, b3, b4, p0, p1, p2, p3, turn, z_hi, z_lo, g, h, lanes, first,
    own_sem, first_sem, send_sem, recv_sem, last_sem,
):
    me = lax.axis_index("pa")
    z, y, x, c = me // 32, (me // 8) % 4, (me // 2) % 4, me % 2
    inputs, outputs = (re_hbm, im_hbm), (out_re, out_im)

    barrier = pltpu.get_barrier_semaphore()
    peers = [device((z + d) % 4, y, x, (c + t) % 2) for t in range(2) for d in (2, 1, 3)]
    peers += [device(z, y, (x + d) % 4, (c + t) % 2) for d in (2, 1, 3, 0) for t in range(2) if d + t]
    peers += [device(z, (y + d) % 4, x, c) for d in (2, 1, 3)]
    for peer in peers:
        pl.semaphore_signal(barrier, inc=1, device_id=(peer,), device_id_type=MESH)
    for part in range(2):

        @pl.loop(0, 8)
        def _(i):
            pltpu.make_async_copy(inputs[part].at[:, :, i * 4, 0], first.at[part, i], first_sem.at[part]).start()

    pl.semaphore_wait(barrier, len(peers))

    def send(src, dst, stage, sem, peer):
        pltpu.make_async_remote_copy(
            src_ref=src, dst_ref=dst, send_sem=send_sem.at[stage], recv_sem=sem, device_id=(peer,), device_id_type=MESH
        ).start()

    def landed(ref, sem):
        pltpu.make_async_remote_copy(
            src_ref=ref, dst_ref=ref, send_sem=sem, recv_sem=sem, device_id=(me,), device_id_type=MESH
        ).wait_recv()

    for part in range(2):
        pltpu.make_async_copy(first.at[part], first.at[part], first_sem.at[part]).wait()
        for d in (2, 1, 3):
            to = (z + d) % 4
            send(first.at[part, :, to], b1.at[0, part, z], 0, recv_sem.at[0, 0], device(to, y, x, c))
    for q in range(1, 4):
        for part in range(2):

            @pl.loop(0, 8)
            def _(i):
                for d in (2, 1, 3):
                    to = (z + d) % 4
                    send(
                        inputs[part].at[to, :, i * 4 + q, 0],
                        b1.at[q, part, z, i],
                        0, recv_sem.at[0, q], device(to, y, x, c),
                    )
                pltpu.make_async_copy(
                    inputs[part].at[z, :, i * 4 + q, 0], b1.at[q, part, z, i], own_sem.at[q]
                ).start()
    for part in range(2):
        b1[0, part, z] = first[part, :, z]

    s = z * 32 + c * 16 + x * 4 + y
    rows = lax.broadcasted_iota(jnp.int32, (128, 128), 0)
    cols = lax.broadcasted_iota(jnp.int32, (128, 128), 1)

    def matrix(phase, bits, scale, table):
        real, imag = unit_root(phase, bits)
        real, imag = real * scale, imag * scale
        for r, k, block in ((0, 0, real), (0, 1, -imag), (1, 0, imag), (1, 1, real)):
            hi, lo = split(block)
            table[r * 128 : r * 128 + 128, k * 128 : k * 128 + 128] = hi
            table[r * 128 + 256 : r * 128 + 384, k * 128 : k * 128 + 128] = lo

    matrix((rows * 128 + s) * cols, 14, 1.0, g)
    target = (rows & 96) + (rows & 3) * 8 + ((rows >> 2) & 3) * 2 + ((rows >> 4) & 1)
    matrix(target * cols, 7, 1.0 / 8192.0, h)
    lane_rows = lax.broadcasted_iota(jnp.int32, (32, 128), 0)
    lane_cols = lax.broadcasted_iota(jnp.int32, (32, 128), 1)
    lanes[0], lanes[1] = unit_root(lane_rows * lane_cols, 12)

    @pl.loop(0, 32)
    def _(f):
        real, imag = unit_root((rows * 128 + s) * (cols + f * 128), 26)
        turn[0, f] = real
        turn[1, f] = imag

    def scalar_root(phase, bits):
        return unit_root(jnp.full((8, 128), 1, jnp.int32) * phase, bits)

    turn_y = [scalar_root(k * y, 4) for k in range(4)]
    turn_x = [scalar_root((4 * k + y) * (2 * x + c), 7) for k in range(4)]

    def four(buf, q, factors):
        @pl.loop(0, 8)
        def _(i):
            v = [tuple(buf[q, p, k, i].reshape(4, 8, 128) for p in range(2)) for k in range(4)]
            v = [times(o, (w[0][None], w[1][None])) for o, w in zip(dft4(v), factors)]
            for k in range(4):
                for p in range(2):
                    buf[q, p, k, i] = v[k][p].reshape(32, 128)

    def step_z(q):
        landed(b1.at[q, :, pl.ds(0, 3)], recv_sem.at[0, q])
        if q:
            pltpu.make_async_copy(b1.at[q, :, 0], b1.at[q, :, 0], own_sem.at[q]).wait()
        four(b1, q, turn_y)
        for d in (2, 1, 3):
            to = (y + d) % 4
            send(b1.at[q, :, to], b2.at[q, :, y], 1, recv_sem.at[1, q], device(z, to, x, c))
        for p in range(2):
            b2[q, p, y] = b1[q, p, y]

    def step_y(q):
        landed(b2.at[q, :, pl.ds(0, 3)], recv_sem.at[1, q])
        four(b2, q, turn_x)
        for d, t in ((2, 1), (2, 0), (1, 1), (3, 1), (1, 0), (3, 0), (0, 1)):
            tx, tc = (x + d) % 4, (c + t) % 2
            send(
                b2.at[q, :, tx, :, pl.ds(pl.multiple_of(tc * 16, 16), 16)],
                b3.at[q, :, x * 2 + c],
                2, recv_sem.at[2, q], device(z, y, tx, tc),
            )
        for p in range(2):
            b3[q, p, x * 2 + c] = b2[q, p, x, :, pl.ds(pl.multiple_of(c * 16, 16), 16)]

    def step_x(q):
        landed(b3.at[q, :, pl.ds(0, 7)], recv_sem.at[2, q])

        @pl.loop(0, 8)
        def _(i):
            v = dft8([(b3[q, 0, k, i], b3[q, 1, k, i]) for k in range(8)])
            for k in range(8):
                b3[q, 0, k, i] = v[k][0]
                b3[q, 1, k, i] = v[k][1]

        def leave_x(tz, tc):
            send(
                b3.at[q, :, tz * 2 + tc],
                b4.at[q, :, :, z * 2 + c],
                3, recv_sem.at[3, q], device(tz, y, x, tc),
            )

        leave_x(z, 1 - c)
        for tc in (1, 0):
            for d in (2, 1, 3):
                leave_x((z + d) % 4, tc)
        for p in range(2):
            b4[q, p, :, z * 2 + c] = b3[q, p, z * 2 + c]

    def step_local(q):
        landed(b4.at[q, :, :, pl.ds(0, 7)], recv_sem.at[3, q])

        @pl.loop(0, 4, unroll=True)
        def _(pair):
            block = jnp.concatenate(
                [
                    jnp.concatenate([b4[q, p, pair * 2 + t].reshape(128, 128) for t in range(2)], axis=1)
                    for p in range(2)
                ],
                axis=0,
            )
            hi, lo = split(block)
            both = jnp.dot(g[...], hi, preferred_element_type=F32)
            result = both[:256] + both[256:] + jnp.dot(g[:256], lo, preferred_element_type=F32)
            for t in range(2):
                f = (pair * 2 + t) * 4 + q
                value = (result[:128, t * 128 : t * 128 + 128], result[128:, t * 128 : t * 128 + 128])
                value = times(value, (turn[0, f], turn[1, f]))
                for p in range(2):
                    b4[q, p, pair * 2 + t] = value[p].reshape(8, 16, 128)

        @pl.loop(0, 8, unroll=True)
        def _(g):
            v = dft8([(b4[q, 0, i, g], b4[q, 1, i, g]) for i in range(8)])
            for i in range(8):
                b4[q, 0, i, g] = v[i][0]
                b4[q, 1, i, g] = v[i][1]

    def finish(j):
        roots = [
            (math.cos(-2 * math.pi * q * j / 32), math.sin(-2 * math.pi * q * j / 32)) for q in range(4)
        ]

        @pl.loop(0, 8, unroll=True)
        def _(g):
            v = [(b4[q, 0, j, g], b4[q, 1, j, g]) for q in range(4)]
            if j:
                v = [v[0]] + [times(v[q], roots[q]) for q in range(1, 4)]
            v = dft4(v)
            where = pl.ds(pl.multiple_of(g * 16, 16), 16)
            for m in range(4):
                row = j + 8 * m
                w = times(v[m], (lanes[0, row : row + 1], lanes[1, row : row + 1]))
                for p in range(2):
                    hi, lo = split(w[p])
                    z_hi[m, where, p * 128 : (p + 1) * 128] = hi
                    z_lo[m, where, p * 128 : (p + 1) * 128] = lo

        flat = p0.at[j].reshape(1024, 128)
        dims = (((1,), (1,)), ((), ()))
        for pair in range(2):
            hi = z_hi[pair * 2 : pair * 2 + 2].reshape(256, 256)
            lo = z_lo[pair * 2 : pair * 2 + 2].reshape(256, 256)
            both = lax.dot_general(h[...], hi, dims, preferred_element_type=F32)
            result = both[:256] + both[256:] + lax.dot_general(h[:256], lo, dims, preferred_element_type=F32)
            for p in range(2):
                for t in range(2):
                    flat[pl.ds(p * 4 + pair * 2 + t, 128, stride=8), :] = result[
                        p * 128 : p * 128 + 128, t * 128 : t * 128 + 128
                    ]

    buffers = (p0, p1, p2, p3)
    nearest = (4 - z) % 4 + 2 * ((3 - z) // 3)
    second = 1 + nearest % 2
    toward = (nearest, second, 6 - nearest - second)

    def leave(j, stage):
        src, dst, sem = buffers[stage].at[j], buffers[stage + 1].at[j], last_sem.at[stage, j]
        axis = ORDERS[j][stage]
        if axis == "z":
            for d in toward:
                to = (z + d) % 4
                send(src.at[to], dst.at[z], 4 + stage, sem, device(to, y, x, c))
            dst[z] = src[z]
        elif axis == "y":
            for d in (2, 1, 3):
                to = (y + d) % 4
                send(src.at[:, :, :, to], dst.at[:, :, :, y], 4 + stage, sem, device(z, to, x, c))
            dst[:, :, :, y] = src[:, :, :, y]
        else:
            send(src.at[:, 1 - c, x], dst.at[:, c, x], 4 + stage, sem, device(z, y, x, 1 - c))
            for tc in (1, 0):
                for d in (2, 1, 3):
                    tx = (x + d) % 4
                    send(src.at[:, tc, tx], dst.at[:, c, x], 4 + stage, sem, device(z, y, tx, tc))
            dst[:, c, x] = src[:, c, x]

    def arrive(j, stage):
        dst, sem = buffers[stage + 1].at[j], last_sem.at[stage, j]
        axis = ORDERS[j][stage]
        if axis == "z":
            landed(dst.at[pl.ds(0, 3)], sem)
        elif axis == "y":
            landed(dst.at[:, :, :, pl.ds(0, 3)], sem)
        else:
            flat = buffers[stage + 1].at[j].reshape(128, 8, 128)
            landed(flat.at[pl.ds(0, 112)], sem)

    def write(j):
        flat = p3.at[j].reshape(1024, 128)
        for p in range(2):
            for m in range(4):
                row = (j + 8 * m) * 128
                outputs[p][row : row + 128] = flat[pl.ds(p * 4 + m, 128, stride=8), :].T

    step_z(0)
    step_z(1)
    step_y(0)
    step_z(2)
    step_y(1)
    step_x(0)
    step_z(3)
    step_y(2)
    step_x(1)
    step_y(3)
    step_x(2)
    step_local(0)
    step_x(3)
    step_local(1)
    step_local(2)
    step_local(3)

    for j in range(8):
        finish(j)
        leave(j, 0)
    def sent(ref, stage):
        pltpu.make_async_remote_copy(
            src_ref=ref, dst_ref=ref, send_sem=send_sem.at[stage], recv_sem=send_sem.at[stage],
            device_id=(me,), device_id_type=MESH,
        ).wait_send()

    def sent_last(stage):
        eighths = sum(7 if order[stage] == "x" else 6 for order in ORDERS)
        sent(p0.reshape(64, 128, 128).at[pl.ds(0, eighths)], 4 + stage)

    for j, stage in ((0, 0), (1, 0), (2, 0), (6, 0), (3, 0), (4, 0), (1, 1), (7, 0), (5, 0), (3, 1), (2, 1), (0, 1), (7, 1), (4, 1), (6, 1), (5, 1), (0, 2), (1, 2), (2, 2), (6, 2), (3, 2), (4, 2), (5, 2), (7, 2)):
        if (j, stage) == (5, 2):
            sent(b1.at[pl.ds(0, 3)], 0)
            sent(b2.at[pl.ds(0, 3)], 1)
            sent(b3.at[:, :, pl.ds(0, 7)], 2)
            sent(b3.at[:, :, pl.ds(0, 7)], 3)
            sent_last(0)
            sent_last(1)
        arrive(j, stage)
        if stage < 2:
            leave(j, stage + 1)
        else:
            write(j)
    sent_last(2)


def store(re_ref, im_ref, out_re, out_im, sems):
    copies = [
        pltpu.make_async_copy(src.at[pl.ds(k * 512, 512)], dst.at[pl.ds(k * 512, 512)], sems.at[p, k])
        for k in range(8)
        for p, (src, dst) in enumerate(((re_ref, out_re), (im_ref, out_im)))
    ]
    for copy in copies:
        copy.start()
    for copy in copies:
        copy.wait()


def body(signal_real, signal_imag):
    shape = (4, 32, 32, 1, 128)
    block = (8, 4, 2, 4, 4, 8, 128)
    spectrum = pl.pallas_call(
        kernel,
        out_shape=[pltpu.VMEM((4096, 128), F32)] * 2,
        in_specs=[pl.BlockSpec(memory_space=pl.ANY)] * 2,
        out_specs=[pl.BlockSpec(memory_space=pltpu.VMEM)] * 2,
        scratch_shapes=[
            pltpu.VMEM((4, 2, 4, 8, 32, 128), F32),
            pltpu.VMEM((4, 2, 4, 8, 32, 128), F32),
            pltpu.VMEM((4, 2, 8, 8, 16, 128), F32),
            pltpu.VMEM((4, 2, 8, 8, 16, 128), F32),
            pltpu.VMEM(block, F32),
            pltpu.VMEM(block, F32),
            pltpu.VMEM(block, F32),
            pltpu.VMEM(block, F32),
            pltpu.VMEM((2, 32, 128, 128), F32),
            pltpu.VMEM((4, 128, 256), BF16),
            pltpu.VMEM((4, 128, 256), BF16),
            pltpu.VMEM((512, 256), BF16),
            pltpu.VMEM((512, 256), BF16),
            pltpu.VMEM((2, 32, 128), F32),
            pltpu.VMEM((2, 8, 4, 32, 128), F32),
            pltpu.SemaphoreType.DMA((4,)),
            pltpu.SemaphoreType.DMA((2,)),
            pltpu.SemaphoreType.DMA((7,)),
            pltpu.SemaphoreType.DMA((4, 4)),
            pltpu.SemaphoreType.DMA((3, 8)),
        ],
        compiler_params=pltpu.CompilerParams(collective_id=0, has_side_effects=True, vmem_limit_bytes=48 * 2**20),
    )(signal_real.reshape(shape), signal_imag.reshape(shape))
    out_re, out_im = pl.pallas_call(
        store,
        out_shape=[jax.ShapeDtypeStruct((4096, 128), F32)] * 2,
        in_specs=[pl.BlockSpec(memory_space=pltpu.VMEM)] * 2,
        out_specs=[pl.BlockSpec(memory_space=pl.ANY)] * 2,
        scratch_shapes=[pltpu.SemaphoreType.DMA((2, 8))],
        compiler_params=pltpu.CompilerParams(vmem_limit_bytes=8 * 2**20),
    )(*spectrum)
    return out_re.reshape(-1), out_im.reshape(-1)


def solution(mesh):
    return jax.shard_map(
        body, mesh=mesh, in_specs=(P("pa"), P("pa")), out_specs=(P("pa"), P("pa")), check_vma=False
    )
```
